32 devices in a mesh: pair: 1 (over z), tp: 4 (over y), side: 8 (over x, core).
Axes of the slice: x: 4, y: 4, z: 1, core: 2. Of those that a mesh axis runs over, the one named last changes fastest.
The devices are a block of a 4x4x8 slice.
Arguments:
- prompt_x: bfloat16 [8192, 2560], P(('pair', 'side'))
- s_len: int32 [8], P(('pair', 'side'))
- w_qkv_pre: bfloat16 [1, 2560, 3, 20, 128], P(None, None, None, 'tp')
- w_out_pre: bfloat16 [1, 20, 128, 2560], P(None, 'tp')
- w_gu_pre: bfloat16 [1, 2, 6912, 2560], P(None, None, 'tp')
- w_down_pre: bfloat16 [1, 6912, 2560], P(None, 'tp')
- gain_pre: float32 [1, 2, 2560], replicated
- dec_tokens: bfloat16 [128, 2560], P(('pair', 'side'))
- k_cache: bfloat16 [1, 128, 256, 5, 4, 128], P(None, ('pair', 'side'), None, None, 'tp')
- v_cache: bfloat16 [1, 128, 256, 5, 4, 128], P(None, ('pair', 'side'), None, None, 'tp')
- c_len: int32 [128], P(('pair', 'side'))
- w_qkv_dec: bfloat16 [1, 2560, 3, 5, 4, 128], P(None, None, None, None, 'tp')
- w_out_dec: bfloat16 [1, 5, 4, 128, 2560], P(None, None, 'tp')
- w_gu_dec: bfloat16 [1, 2, 6912, 2560], P(None, None, 'tp')
- w_down_dec: bfloat16 [1, 6912, 2560], P(None, 'tp')
- gain_dec: float32 [1, 2, 2560], replicated
Outputs:
- output 1: bfloat16 [8192, 2560], P(('pair', 'side'))
- output 2: bfloat16 [128, 2560], P(('pair', 'side'))
- output 3: bfloat16 [1, 8192, 5, 4, 128], P(None, ('pair', 'side'), None, 'tp')
- output 4: bfloat16 [1, 8192, 5, 4, 128], P(None, ('pair', 'side'), None, 'tp')
- output 5: bfloat16 [1, 128, 256, 5, 4, 128], P(None, ('pair', 'side'), None, None, 'tp')
- output 6: bfloat16 [1, 128, 256, 5, 4, 128], P(None, ('pair', 'side'), None, None, 'tp')
All inputs are finite; a program needn't handle non-finite values.
Results may differ from the reference program's by a relative error of at most 0.0126162.
Values are sent between devices in bfloat16 or wider.
A program may use at most 768 MiB of HBM per device.

```python
import jax
import jax.numpy as jnp
from jax import lax

D = 2560
HEADS = 20
HEAD = 128
FF = 6912
LAYERS = 1
PROMPT = 1024
BATCH = 16
CACHE = 256
TP_SIZE = 4
SIDES = 8

EPSILON = 1e-6
THETA = 10000.0
QK_GAIN = 1.5
OUT_GAIN = 2.0
MASKED = -1e30


def draw_int_inputs(len_key, cache_key):
    low_prompt = PROMPT // 2
    len_keys = jax.random.split(len_key, 2)
    s_len = jax.random.randint(len_keys[0], (SIDES,), low_prompt, PROMPT + 1, dtype=jnp.int32)
    slot_top = jax.random.randint(len_keys[1], (), 0, SIDES, dtype=jnp.int32)
    s_len = s_len.at[slot_top].set(PROMPT).at[(slot_top + 1) % SIDES].set(low_prompt)
    low_cache = CACHE // 4
    row_total = SIDES * BATCH
    cache_keys = jax.random.split(cache_key, 2)
    c_len = jax.random.randint(cache_keys[0], (row_total,), low_cache, CACHE, dtype=jnp.int32)
    row_top = jax.random.randint(cache_keys[1], (), 0, row_total, dtype=jnp.int32)
    c_len = c_len.at[row_top].set(CACHE - 1).at[(row_top + 1) % row_total].set(low_cache)
    return s_len, c_len


def draw_weights(weight_key):
    weight_keys = jax.random.split(weight_key, 5)
    qkv_scale = jnp.array([QK_GAIN, QK_GAIN, 1.0], jnp.float32)[:, None, None] * D ** -0.5
    w_qkv = (jax.random.normal(weight_keys[0], (LAYERS, D, 3, HEADS, HEAD), jnp.float32) * qkv_scale).astype(jnp.bfloat16)
    w_out = (jax.random.normal(weight_keys[1], (LAYERS, HEADS, HEAD, D), jnp.float32) * (OUT_GAIN * (HEADS * HEAD) ** -0.5)).astype(jnp.bfloat16)
    w_gu = (jax.random.normal(weight_keys[2], (LAYERS, 2, FF, D), jnp.float32) * D ** -0.5).astype(jnp.bfloat16)
    w_down = (jax.random.normal(weight_keys[3], (LAYERS, FF, D), jnp.float32) * FF ** -0.5).astype(jnp.bfloat16)
    gains = jax.random.uniform(weight_keys[4], (LAYERS, 2, D), jnp.float32, 0.5, 1.5)
    return w_qkv, w_out, w_gu, w_down, gains


def setup_inputs(seed: int = 0, part: int = 0) -> dict:
    shared_keys = jax.random.split(jax.random.key(seed + 1), 2)
    part_keys = jax.random.split(jax.random.fold_in(jax.random.key(seed), part), 6)
    heads_tp = HEADS // TP_SIZE
    w_qkv_pre, w_out_pre, w_gu_pre, w_down_pre, gain_pre = draw_weights(shared_keys[0])
    w_qkv_dec, w_out_dec, w_gu_dec, w_down_dec, gain_dec = draw_weights(shared_keys[1])
    s_len, c_len = draw_int_inputs(part_keys[0], part_keys[1])
    prompt_x = jax.random.normal(part_keys[2], (SIDES * PROMPT, D), jnp.float32).astype(jnp.bfloat16)
    dec_tokens = jax.random.normal(part_keys[3], (SIDES * BATCH, D), jnp.float32).astype(jnp.bfloat16)
    cache_shape = (LAYERS, SIDES * BATCH, CACHE, heads_tp, TP_SIZE, HEAD)
    k_cache = (jax.random.normal(part_keys[4], cache_shape, jnp.float32) * QK_GAIN).astype(jnp.bfloat16)
    v_cache = jax.random.normal(part_keys[5], cache_shape, jnp.float32).astype(jnp.bfloat16)
    return {'prompt_x': prompt_x, 's_len': s_len, 'w_qkv_pre': w_qkv_pre, 'w_out_pre': w_out_pre, 'w_gu_pre': w_gu_pre, 'w_down_pre': w_down_pre, 'gain_pre': gain_pre, 'dec_tokens': dec_tokens, 'k_cache': k_cache, 'v_cache': v_cache, 'c_len': c_len, 'w_qkv_dec': w_qkv_dec.reshape(LAYERS, D, 3, heads_tp, TP_SIZE, HEAD), 'w_out_dec': w_out_dec.reshape(LAYERS, heads_tp, TP_SIZE, HEAD, D), 'w_gu_dec': w_gu_dec, 'w_down_dec': w_down_dec, 'gain_dec': gain_dec}


def rms_norm(hidden, gain_vec):
    hid_f32 = hidden.astype(jnp.float32)
    inv_rms = lax.rsqrt(jnp.mean(hid_f32 * hid_f32, axis=-1, keepdims=True) + EPSILON)
    return (hid_f32 * inv_rms * gain_vec).astype(jnp.bfloat16)


def add_residual(hidden, update):
    return (hidden.astype(jnp.float32) + update.astype(jnp.float32)).astype(jnp.bfloat16)


def rope_tables(positions):
    half_dim = HEAD // 2
    inv_freq = THETA ** (-jnp.arange(half_dim, dtype=jnp.float32) * 2.0 / HEAD)
    angles = positions.astype(jnp.float32)[:, None] * inv_freq[None, :]
    return jnp.cos(angles), jnp.sin(angles)


def apply_rope(values_in, cos_tab, sin_tab):
    half_dim = values_in.shape[-1] // 2
    lower_half = values_in[..., :half_dim]
    upper_half = values_in[..., half_dim:]
    cos_b = cos_tab[:, None, :]
    sin_b = sin_tab[:, None, :]
    return jnp.concatenate([lower_half * cos_b - upper_half * sin_b, upper_half * cos_b + lower_half * sin_b], axis=-1)


def mlp_block(hidden, gain_vec, w_gu, w_down):
    normed = rms_norm(hidden, gain_vec)
    gate_up = jnp.einsum('sd,kfd->skf', normed.astype(jnp.float32), w_gu.astype(jnp.float32))
    gate_val = gate_up[:, 0].astype(jnp.bfloat16).astype(jnp.float32)
    up_val = gate_up[:, 1].astype(jnp.bfloat16).astype(jnp.float32)
    activated = (jax.nn.silu(gate_val) * up_val).astype(jnp.bfloat16)
    down_out = jnp.dot(activated, w_down, preferred_element_type=jnp.float32).astype(jnp.bfloat16)
    return add_residual(hidden, down_out)


def prefill_one(x_inst, s_valid, w_qkv, w_out, w_gu, w_down, gains):
    positions = jnp.arange(PROMPT)
    cos_tab, sin_tab = rope_tables(positions)
    allowed = (positions[None, :] <= positions[:, None]) & (positions[None, :] < s_valid)

    def head_attention(head_in):
        q_head, k_head, v_head = head_in
        scores = jnp.einsum('qe,ke->qk', q_head.astype(jnp.float32), k_head.astype(jnp.float32)) * HEAD ** -0.5
        scores = jnp.where(allowed, scores, MASKED)
        prob_bf = jax.nn.softmax(scores, axis=-1).astype(jnp.bfloat16)
        return jnp.einsum('qk,ke->qe', prob_bf.astype(jnp.float32), v_head.astype(jnp.float32)).astype(jnp.bfloat16)

    def layer_step(hidden, layer_in):
        wqkv_l, wout_l, wgu_l, wdown_l, gain_l = layer_in
        normed = rms_norm(hidden, gain_l[0])
        qkv_out = jnp.einsum('sd,dkhe->skhe', normed.astype(jnp.float32), wqkv_l.astype(jnp.float32))
        queries = apply_rope(qkv_out[:, 0], cos_tab, sin_tab).astype(jnp.bfloat16)
        keys_new = apply_rope(qkv_out[:, 1], cos_tab, sin_tab).astype(jnp.bfloat16)
        values_new = qkv_out[:, 2].astype(jnp.bfloat16)
        context = lax.map(head_attention, (queries.transpose(1, 0, 2), keys_new.transpose(1, 0, 2), values_new.transpose(1, 0, 2)))
        attn_out = jnp.einsum('hse,hed->sd', context.astype(jnp.float32), wout_l.astype(jnp.float32)).astype(jnp.bfloat16)
        hidden = add_residual(hidden, attn_out)
        hidden = mlp_block(hidden, gain_l[1], wgu_l, wdown_l)
        return hidden, (keys_new, values_new)

    return lax.scan(layer_step, x_inst, (w_qkv, w_out, w_gu, w_down, gains))


def decode_rows(tokens, k_cache, v_cache, c_len, w_qkv, w_out, w_gu, w_down, gains):
    row_total = tokens.shape[0]
    cos_tab, sin_tab = rope_tables(c_len)
    cache_pos = jnp.arange(CACHE)
    k_flat = k_cache.reshape(LAYERS, row_total, CACHE, HEADS, HEAD)
    v_flat = v_cache.reshape(LAYERS, row_total, CACHE, HEADS, HEAD)
    wqkv_flat = w_qkv.reshape(LAYERS, D, 3, HEADS, HEAD)
    wout_flat = w_out.reshape(LAYERS, HEADS, HEAD, D)
    write_at = (cache_pos[None, :] == c_len[:, None])[:, :, None, None]

    def row_attention(row_in):
        q_row, k_row, v_row, kc_row, vc_row, len_row = row_in
        cache_scores = jnp.einsum('he,the->ht', q_row.astype(jnp.float32), kc_row.astype(jnp.float32)) * HEAD ** -0.5
        cache_scores = jnp.where(cache_pos[None, :] < len_row, cache_scores, MASKED)
        self_score = jnp.sum(q_row.astype(jnp.float32) * k_row.astype(jnp.float32), axis=-1) * HEAD ** -0.5
        joint_scores = jnp.concatenate([cache_scores, self_score[:, None]], axis=1)
        prob_bf = jax.nn.softmax(joint_scores, axis=-1).astype(jnp.bfloat16).astype(jnp.float32)
        context = jnp.einsum('ht,the->he', prob_bf[:, :CACHE], vc_row.astype(jnp.float32)) + prob_bf[:, CACHE:] * v_row.astype(jnp.float32)
        return context.astype(jnp.bfloat16)

    def layer_step(hidden, layer_in):
        wqkv_l, wout_l, wgu_l, wdown_l, gain_l, kc_l, vc_l = layer_in
        normed = rms_norm(hidden, gain_l[0])
        qkv_out = jnp.einsum('bd,dkhe->bkhe', normed.astype(jnp.float32), wqkv_l.astype(jnp.float32))
        queries = apply_rope(qkv_out[:, 0], cos_tab, sin_tab).astype(jnp.bfloat16)
        k_tok = apply_rope(qkv_out[:, 1], cos_tab, sin_tab).astype(jnp.bfloat16)
        v_tok = qkv_out[:, 2].astype(jnp.bfloat16)
        context = lax.map(row_attention, (queries, k_tok, v_tok, kc_l, vc_l, c_len))
        attn_out = jnp.einsum('bhe,hed->bd', context.astype(jnp.float32), wout_l.astype(jnp.float32)).astype(jnp.bfloat16)
        hidden = add_residual(hidden, attn_out)
        hidden = mlp_block(hidden, gain_l[1], wgu_l, wdown_l)
        kc_next = jnp.where(write_at, k_tok[:, None], kc_l)
        vc_next = jnp.where(write_at, v_tok[:, None], vc_l)
        return hidden, (kc_next, vc_next)

    final_tokens, (kc_all, vc_all) = lax.scan(layer_step, tokens, (wqkv_flat, wout_flat, w_gu, w_down, gains, k_flat, v_flat))
    return final_tokens, kc_all.reshape(k_cache.shape), vc_all.reshape(v_cache.shape)


def reference(prompt_x, s_len, w_qkv_pre, w_out_pre, w_gu_pre, w_down_pre, gain_pre, dec_tokens, k_cache, v_cache, c_len, w_qkv_dec, w_out_dec, w_gu_dec, w_down_dec, gain_dec):
    prompts = prompt_x.reshape(SIDES, PROMPT, D)

    def run_instance(inst_in):
        x_inst, s_valid = inst_in
        final_hidden, (k_all, v_all) = prefill_one(x_inst, s_valid, w_qkv_pre, w_out_pre, w_gu_pre, w_down_pre, gain_pre)
        return final_hidden, k_all, v_all

    final_hidden, k_all, v_all = lax.map(run_instance, (prompts, s_len))
    half_sides = SIDES // 2
    prompt_shape = (LAYERS, SIDES * PROMPT, HEADS // TP_SIZE, TP_SIZE, HEAD)
    k_prompt = jnp.roll(k_all, half_sides, axis=0).transpose(1, 0, 2, 3, 4).reshape(prompt_shape)
    v_prompt = jnp.roll(v_all, half_sides, axis=0).transpose(1, 0, 2, 3, 4).reshape(prompt_shape)
    dec_out, k_cache_new, v_cache_new = decode_rows(dec_tokens, k_cache, v_cache, c_len, w_qkv_dec, w_out_dec, w_gu_dec, w_down_dec, gain_dec)
    return (final_hidden.reshape(SIDES * PROMPT, D), dec_out, k_prompt, v_prompt, k_cache_new, v_cache_new)
```

```python
import functools

import jax
import jax.numpy as jnp
from jax import lax
from jax.experimental import pallas as pl
from jax.experimental.pallas import tpu as pltpu
from jax.sharding import PartitionSpec as P

EPSILON = 1e-6
THETA = 10000.0
MASKED = -1e30
VMEM_LIMIT = 60 * 1024 * 1024
ANY = pl.BlockSpec(memory_space=pl.ANY)
VM = pl.BlockSpec(memory_space=pltpu.VMEM)
SM = pl.BlockSpec(memory_space=pltpu.SMEM)


def rms_norm(hidden, gain_vec):
    hid_f32 = hidden.astype(jnp.float32)
    inv_rms = lax.rsqrt(jnp.mean(hid_f32 * hid_f32, axis=-1, keepdims=True) + EPSILON)
    return (hid_f32 * inv_rms * gain_vec).astype(jnp.bfloat16)


def add_residual(hidden, update):
    return (hidden.astype(jnp.float32) + update.astype(jnp.float32)).astype(jnp.bfloat16)


def rope_tables(positions, head_dim):
    half_dim = head_dim // 2
    inv_freq = THETA ** (-jnp.arange(half_dim, dtype=jnp.float32) * 2.0 / head_dim)
    angles = positions.astype(jnp.float32)[:, None] * inv_freq[None, :]
    return jnp.cos(angles), jnp.sin(angles)


def apply_rope(values_in, cos_tab, sin_tab):
    half_dim = values_in.shape[-1] // 2
    lower_half = values_in[..., :half_dim]
    upper_half = values_in[..., half_dim:]
    cos_b = cos_tab[:, None, :]
    sin_b = sin_tab[:, None, :]
    return jnp.concatenate([lower_half * cos_b - upper_half * sin_b, upper_half * cos_b + lower_half * sin_b], axis=-1)


def front_kernel(len_ref, cos_ref, sin_ref, g1_ref, g2_ref, x_hbm, wqkv_hbm, wo_hbm, h_hbm, n_hbm, k_ref, v_ref, xs, ns, nv, wv, acc, qv, ctx, wo, wsem, xsem, osem, hsem, nsem, ssem, rsem, *, rb, tp_size, side_size):
    n_kind, heads, depth, head_dim = wqkv_hbm.shape
    rows = x_hbm.shape[0]
    n_blk = rows // rb
    shard = heads * head_dim
    width = n_kind * shard
    half = depth // 2
    me = lax.axis_index('tp')
    side = lax.axis_index('side')
    core = lax.rem(side, 2)
    chip = side // 2
    n_chip = side_size // 2
    part = shard // side_size
    tp_of = lambda d: lax.rem(me + d + tp_size, tp_size)
    chip_of = lambda d: lax.rem(chip + d + n_chip, n_chip)
    to_right = {'tp': tp_of(1)}
    to_left = {'tp': tp_of(-1)}
    to_up = {'side': chip_of(1) * 2 + core}
    to_down = {'side': chip_of(-1) * 2 + core}
    to_twin = {'side': chip * 2 + 1 - core}
    whole = pl.ds(0, depth)
    cols_a = pl.ds(0, half)
    cols_b = pl.ds(half, half)

    def send(idx, ref, dev, src=None):
        return pltpu.make_async_remote_copy(src_ref=ref if src is None else src, dst_ref=ref, send_sem=ssem.at[idx], recv_sem=rsem.at[idx], device_id=dev, device_id_type=pl.DeviceIdType.MESH)

    def w_part(d_tp, d_chip, cols, core_id):
        row0 = pl.multiple_of((chip_of(d_chip) * 2 + core_id) * part, 16)
        return wo.at[tp_of(d_tp), pl.ds(row0, part), cols]

    def c_part(d_tp, blk):
        return ctx.at[pl.ds(blk * rb, rb), pl.ds(pl.multiple_of(tp_of(d_tp) * shard, 128), shard)]

    offs = (-1, 1, 2)
    hops = (0, -1, 1, 2)
    sent = []

    def start(copy):
        copy.start()
        sent.append(copy)

    own_slice = wo_hbm.at[pl.ds(pl.multiple_of(side * part, 16), part), :]
    y_send = [
        lambda: send(0, w_part(0, 0, whole, core), to_right, src=own_slice),
        lambda: send(1, w_part(0, 0, whole, core), to_left, src=own_slice),
        lambda: send(2, w_part(-1, 0, cols_a, core), to_right),
        lambda: send(3, w_part(1, 0, cols_b, core), to_left),
    ]
    y_land = [
        lambda: send(0, w_part(-1, 0, whole, core), to_right),
        lambda: send(1, w_part(1, 0, whole, core), to_left),
        lambda: send(2, w_part(-2, 0, cols_a, core), to_right),
        lambda: send(3, w_part(2, 0, cols_b, core), to_left),
    ]

    def x_send(i, kind):
        d = offs[i]
        idx = 4 + 4 * i + kind
        if kind == 0:
            return send(idx, w_part(d, 0, whole, core), to_up)
        if kind == 1:
            return send(idx, w_part(d, 0, whole, core), to_down)
        if kind == 2:
            return send(idx, w_part(d, -1, cols_a, core), to_up)
        return send(idx, w_part(d, 1, cols_b, core), to_down)

    def x_land(i, kind):
        d = offs[i]
        idx = 4 + 4 * i + kind
        if kind == 0:
            return send(idx, w_part(d, -1, whole, core), to_up)
        if kind == 1:
            return send(idx, w_part(d, 1, whole, core), to_down)
        if kind == 2:
            return send(idx, w_part(d, -2, cols_a, core), to_up)
        return send(idx, w_part(d, 2, cols_b, core), to_down)

    def t_send(i, j):
        return send(16 + 4 * i + j, w_part(offs[i], hops[j], whole, core), to_twin)

    def t_land(i, j):
        return send(16 + 4 * i + j, w_part(offs[i], hops[j], whole, 1 - core), to_twin)

    c_right = lambda blk: send(28 + blk, c_part(0, blk), to_right)
    c_left = lambda blk: send(28 + n_blk + blk, c_part(0, blk), to_left)
    c_from_left = lambda blk: send(28 + blk, c_part(-1, blk), to_right)
    c_from_right = lambda blk: send(28 + n_blk + blk, c_part(1, blk), to_left)

    def f_send(blk):
        if blk < n_blk // 2:
            return send(28 + 2 * n_blk + blk, c_part(-1, blk), to_right)
        return send(28 + 2 * n_blk + blk, c_part(1, blk), to_left)

    def f_land(blk):
        return send(28 + 2 * n_blk + blk, c_part(2, blk), to_right if blk < n_blk // 2 else to_left)

    def w_copy(kind, head):
        idx = kind * heads + head
        return pltpu.make_async_copy(wqkv_hbm.at[kind, head], wv.at[:, pl.ds(idx * head_dim, head_dim)], wsem.at[idx])

    x_in = lambda blk: pltpu.make_async_copy(x_hbm.at[pl.ds(blk * rb, rb), :], nv.at[pl.ds(blk * rb, rb), :], xsem.at[blk])
    x_again = lambda blk: pltpu.make_async_copy(x_hbm.at[pl.ds(blk * rb, rb), :], xs.at[blk % 2], xsem.at[n_blk + blk])
    own_w = pltpu.make_async_copy(wo_hbm, wo.at[me], osem.at[0])

    for blk in range(n_blk):
        x_in(blk).start()
    for kind in range(n_kind):
        for head in range(heads):
            w_copy(kind, head).start()
    own_w.start()
    x_again(0).start()
    x_again(1).start()

    barrier = pltpu.get_barrier_semaphore()
    for dev in (to_right, to_left, to_up, to_down, to_twin):
        pl.semaphore_signal(barrier, inc=1, device_id=dev, device_id_type=pl.DeviceIdType.MESH)
    pl.semaphore_wait(barrier, 5)
    start(y_send[0]())
    start(y_send[1]())

    nb = 64
    for blk in range(n_blk):
        x_in(blk).wait()

    def norm_step(i, carry):
        r = pl.ds(pl.multiple_of(i * nb, nb), nb)
        nv[r, :] = rms_norm(nv[r, :], g1_ref[...])
        return carry

    lax.fori_loop(0, rows // nb, norm_step, 0)
    for kind in range(n_kind):
        for head in range(heads):
            w_copy(kind, head).wait()

    def qkv_step(i, carry):
        r = pl.ds(pl.multiple_of(i * rb, rb), rb)
        acc[pl.ds(0, rb), pl.ds(0, width)] = jnp.dot(nv[r, :], wv[...], preferred_element_type=jnp.float32)
        cos_b = cos_ref[r, :]
        sin_b = sin_ref[r, :]
        for head in range(heads):
            for kind, out in ((0, qv), (1, k_ref)):
                idx = (kind * heads + head) * head_dim
                val = acc[0:rb, idx:idx + head_dim]
                out[head, r, :] = (val * cos_b + pltpu.roll(val, head_dim // 2, 1) * sin_b).astype(jnp.bfloat16)
            idx = (2 * heads + head) * head_dim
            v_ref[head, r, :] = acc[0:rb, idx:idx + head_dim].astype(jnp.bfloat16)
        return carry

    lax.fori_loop(0, n_blk // 2, qkv_step, 0)
    for m in range(2):
        y_land[m]().wait_recv()
    for m in range(2):
        start(y_send[2 + m]())
    for i in range(2):
        start(x_send(i, 0))
        start(x_send(i, 1))
        start(t_send(i, 0))
    lax.fori_loop(n_blk // 2, n_blk, qkv_step, 0)
    for m in range(2):
        y_land[2 + m]().wait_recv()
    start(x_send(2, 0))
    start(x_send(2, 1))
    start(t_send(2, 0))

    valid = len_ref[0]
    scale = head_dim ** -0.5
    for blk in range(n_blk):
        span = (blk + 1) * rb
        rowi = lax.broadcasted_iota(jnp.int32, (rb, span), 0) + blk * rb
        coli = lax.broadcasted_iota(jnp.int32, (rb, span), 1)
        seen = (coli <= rowi) & (coli < valid)

        def head_step(head, carry, blk=blk, span=span, seen=seen):
            kk = k_ref[head, pl.ds(0, span), :]
            s = lax.dot_general(qv[head, pl.ds(blk * rb, rb), :], kk, (((1,), (1,)), ((), ())), preferred_element_type=jnp.float32)
            s = jnp.where(seen, s * scale, MASKED)
            p = jnp.exp(s - jnp.max(s, axis=-1, keepdims=True))
            p = (p * (1.0 / jnp.sum(p, axis=-1, keepdims=True))).astype(jnp.bfloat16)
            c = jnp.dot(p, v_ref[head, pl.ds(0, span), :], preferred_element_type=jnp.float32).astype(jnp.bfloat16)
            ctx[pl.ds(blk * rb, rb), pl.ds(pl.multiple_of(me * shard + head * head_dim, head_dim), head_dim)] = c
            return carry

        lax.fori_loop(0, heads, head_step, 0)
        start(c_right(blk))
        start(c_left(blk))

    def relay_x(i):
        for kind in range(2):
            x_land(i, kind).wait_recv()
        for kind in range(2):
            start(x_send(i, 2 + kind))
        start(t_send(i, 1))
        start(t_send(i, 2))

    relay_x(0)
    relay_x(1)
    own_w.wait()

    def add_shard(d, first):
        w_ref = wo.at[tp_of(d)]
        col = pl.ds(pl.multiple_of(tp_of(d) * shard, 128), shard)

        def step(i, carry):
            r = pl.ds(pl.multiple_of(i * rb, rb), rb)
            val = jnp.dot(ctx[r, col], w_ref[...], preferred_element_type=jnp.float32)
            if first:
                acc[r, :] = val
            else:
                acc[r, :] += val
            return carry

        lax.fori_loop(0, n_blk, step, 0)

    for blk in range(n_blk // 2):
        c_from_left(blk).wait_recv()
        start(f_send(blk))
    for blk in range(n_blk // 2, n_blk):
        c_from_right(blk).wait_recv()
        start(f_send(blk))
    add_shard(0, True)
    relay_x(2)
    for i in range(3):
        for kind in range(2, 4):
            x_land(i, kind).wait_recv()
        start(t_send(i, 3))
    for i in range(3):
        for j in range(4):
            t_land(i, j).wait_recv()
    for blk in range(n_blk // 2, n_blk):
        c_from_left(blk).wait_recv()
    for blk in range(n_blk // 2):
        c_from_right(blk).wait_recv()
    add_shard(-1, False)
    add_shard(1, False)

    col = pl.ds(pl.multiple_of(tp_of(2) * shard, 128), shard)
    h_copy = lambda blk: pltpu.make_async_copy(nv.at[pl.ds(blk * rb, rb), :], h_hbm.at[pl.ds(blk * rb, rb), :], hsem.at[blk])
    n_copy = lambda blk: pltpu.make_async_copy(ns.at[blk % 2], n_hbm.at[pl.ds(blk * rb, rb), :], nsem.at[blk])
    w_far = wo.at[tp_of(2)]
    for blk in range(n_blk):
        f_land(blk).wait_recv()
        x_again(blk).wait()
        if blk >= 2:
            n_copy(blk - 2).wait()
        r = pl.ds(blk * rb, rb)
        acc[r, :] += jnp.dot(ctx[r, col], w_far[...], preferred_element_type=jnp.float32)

        def end_step(i, carry, blk=blk):
            r = pl.ds(pl.multiple_of(blk * rb + i * nb, nb), nb)
            q = pl.ds(pl.multiple_of(i * nb, nb), nb)
            h = add_residual(xs[blk % 2, q, :], acc[r, :].astype(jnp.bfloat16))
            nv[r, :] = h
            ns[blk % 2, q, :] = rms_norm(h, g2_ref[...])
            return carry

        lax.fori_loop(0, rb // nb, end_step, 0)
        h_copy(blk).start()
        n_copy(blk).start()
        if blk + 2 < n_blk:
            x_again(blk + 2).start()
    for blk in range(n_blk):
        h_copy(blk).wait()
        if blk >= n_blk - 2:
            n_copy(blk).wait()
    for copy in sent:
        copy.wait_send()


def front_call(x, s_len, gain1, gain2, cos_full, sin_full, w_qkv, w_o, tp_size, side_size):
    rows, depth = x.shape
    n_kind, heads, _, head_dim = w_qkv.shape
    shard = heads * head_dim
    width = n_kind * shard
    rb = 256
    n_blk = rows // rb
    n_msg = 28 + 3 * n_blk
    act = jax.ShapeDtypeStruct((rows, depth), jnp.bfloat16)
    kv = jax.ShapeDtypeStruct((heads, rows, head_dim), jnp.bfloat16)
    dma = pltpu.SemaphoreType.DMA
    return pl.pallas_call(
        functools.partial(front_kernel, rb=rb, tp_size=tp_size, side_size=side_size),
        out_shape=(act, act, kv, kv),
        in_specs=[SM, VM, VM, VM, VM, ANY, ANY, ANY],
        out_specs=(ANY, ANY, VM, VM),
        scratch_shapes=[
            pltpu.VMEM((2, rb, depth), jnp.bfloat16),
            pltpu.VMEM((2, rb, depth), jnp.bfloat16),
            pltpu.VMEM((rows, depth), jnp.bfloat16),
            pltpu.VMEM((depth, width), jnp.bfloat16),
            pltpu.VMEM((rows, depth), jnp.float32),
            pltpu.VMEM((heads, rows, head_dim), jnp.bfloat16),
            pltpu.VMEM((rows, tp_size * shard), jnp.bfloat16),
            pltpu.VMEM((tp_size, shard, depth), jnp.bfloat16),
            dma((n_kind * heads,)), dma((2 * n_blk,)), dma((1,)), dma((n_blk,)), dma((n_blk,)), dma((n_msg,)), dma((n_msg,)),
        ],
        compiler_params=pltpu.CompilerParams(vmem_limit_bytes=67043328, collective_id=0, has_side_effects=True),
        cost_estimate=pl.CostEstimate(flops=2 * rows * depth * (width + tp_size * shard), bytes_accessed=2 * (4 * rows * depth + depth * width), transcendentals=0),
        name="front",
    )(s_len, cos_full, sin_full, gain1, gain2, x, w_qkv, w_o)


def mlp_kernel(idx_ref, n_hbm, wgu_hbm, wd_hbm, o0, o1, o2, o3, nv, gu_v, wd_v, acc, nsem, gsem, dsem, *, fb):
    ff, depth = wd_hbm.shape
    chunk = o0.shape[0]
    pieces = [(f, min(fb, ff - f)) for f in range(0, ff, fb)]

    def n_copy(c):
        src = n_hbm.at[pl.ds(pl.multiple_of(idx_ref[c] * chunk, chunk), chunk), :]
        return pltpu.make_async_copy(src, nv.at[pl.ds(c * chunk, chunk), :], nsem.at[c])

    def gu_copy(p, which):
        f, size = pieces[p]
        return pltpu.make_async_copy(wgu_hbm.at[which, pl.ds(f, size), :], gu_v.at[which, pl.ds(f, size), :], gsem.at[2 * p + which])

    def wd_copy(p):
        f, size = pieces[p]
        return pltpu.make_async_copy(wd_hbm.at[pl.ds(f, size), :], wd_v.at[pl.ds(f, size), :], dsem.at[p])

    n_copy(0).start()
    n_copy(1).start()
    for p in range(len(pieces)):
        gu_copy(p, 0).start()
        gu_copy(p, 1).start()
    for p in range(len(pieces)):
        wd_copy(p).start()
    n_copy(0).wait()
    n_copy(1).wait()
    nt = (((1,), (1,)), ((), ()))
    for p, (f, size) in enumerate(pieces):
        gu_copy(p, 0).wait()
        gu_copy(p, 1).wait()
        gate = lax.dot_general(nv[...], gu_v[0, f:f + size, :], nt, preferred_element_type=jnp.float32)
        up = lax.dot_general(nv[...], gu_v[1, f:f + size, :], nt, preferred_element_type=jnp.float32)
        gate = gate.astype(jnp.bfloat16).astype(jnp.float32)
        up = up.astype(jnp.bfloat16).astype(jnp.float32)
        acc[:, f:f + size] = (gate * jax.nn.sigmoid(gate) * up).astype(jnp.bfloat16)
    for p in range(len(pieces)):
        wd_copy(p).wait()
    half = depth // 2
    for lo, top, low in ((0, o0, o2), (half, o1, o3)):
        for c in range(0, half, fb):
            part = jnp.dot(acc[...], wd_v[:, lo + c:lo + c + fb], preferred_element_type=jnp.float32)
            top[:, c:c + fb] = part[:chunk]
            low[:, c:c + fb] = part[chunk:]


def mlp_call(idx, normed, w_gu, w_down, chunk):
    ff, depth = w_down.shape
    fb = 256
    n_piece = -(-ff // fb)
    out = jax.ShapeDtypeStruct((chunk, depth // 2), jnp.float32)
    return pl.pallas_call(
        functools.partial(mlp_kernel, fb=fb),
        out_shape=(out,) * 4,
        in_specs=[SM, ANY, ANY, ANY],
        out_specs=(VM,) * 4,
        scratch_shapes=[
            pltpu.VMEM((2 * chunk, depth), jnp.bfloat16),
            pltpu.VMEM((2, ff, depth), jnp.bfloat16),
            pltpu.VMEM((ff, depth), jnp.bfloat16),
            pltpu.VMEM((2 * chunk, ff), jnp.bfloat16),
            pltpu.SemaphoreType.DMA((2,)),
            pltpu.SemaphoreType.DMA((2 * n_piece,)),
            pltpu.SemaphoreType.DMA((n_piece,)),
        ],
        compiler_params=pltpu.CompilerParams(vmem_limit_bytes=VMEM_LIMIT),
        cost_estimate=pl.CostEstimate(flops=12 * chunk * ff * depth, bytes_accessed=6 * ff * depth + 12 * chunk * depth, transcendentals=0),
        name="mlp",
    )(idx, normed, w_gu, w_down)


def assemble_kernel(own, left, right, top, low, out, sems, *, tp_size):
    rows = own.shape[0]
    half = rows // 2
    me = lax.axis_index('tp')
    spot = lambda d, off: pl.multiple_of(lax.rem(me + d + tp_size, tp_size) * rows + off, half)
    places = ((own, 0, 0, rows), (left, -1, 0, rows), (right, 1, 0, rows), (top, 2, 0, half), (low, 2, half, half))
    copies = [pltpu.make_async_copy(ref, out.at[pl.ds(spot(d, off), size), :], sems.at[n]) for n, (ref, d, off, size) in enumerate(places)]
    for copy in copies:
        copy.start()
    for copy in copies:
        copy.wait()


def assemble_call(own, left, right, top, low, tp_size):
    rows, width = own.shape
    return pl.pallas_call(
        functools.partial(assemble_kernel, tp_size=tp_size),
        out_shape=jax.ShapeDtypeStruct((tp_size * rows, width), own.dtype),
        in_specs=[VM] * 5,
        out_specs=ANY,
        scratch_shapes=[pltpu.SemaphoreType.DMA((5,))],
        compiler_params=pltpu.CompilerParams(vmem_limit_bytes=32 * 1024 * 1024),
        cost_estimate=pl.CostEstimate(flops=rows * width, bytes_accessed=16 * rows * width, transcendentals=0),
        name="assemble",
    )(own, left, right, top, low)


def ring_gather(block, right, left, me, tp_size):
    rows = block.shape[0]
    half = rows // 2
    from_left = lax.ppermute(block, 'tp', right)
    from_right = lax.ppermute(block, 'tp', left)
    far_top = lax.ppermute(from_left[:half], 'tp', right)
    far_low = lax.ppermute(from_right[half:], 'tp', left)
    return assemble_call(block, from_left, from_right, far_top, far_low, tp_size)


def move_kv(k, v, me, tp_size, side_size):
    heads = k.shape[0]
    kv = jnp.stack([k, v], axis=1)
    pieces = []
    for off in range(tp_size):
        group = list(range(off, heads, tp_size))
        perm = []
        for t in range(tp_size):
            for s in range(side_size):
                perm.append((t * side_size + s, (t + off) % tp_size * side_size + (s + side_size // 2) % side_size))
        got = lax.ppermute(jnp.stack([kv[i] for i in group]), ('tp', 'side'), perm)
        pieces.extend((group[n], got[n]) for n in range(len(group)))
    stacked = jnp.stack([piece for _, piece in sorted(pieces, key=lambda item: item[0])])
    head_ids = jnp.arange(heads) * tp_size + me
    picked = jnp.take(stacked, head_ids % heads, axis=0)
    return picked[:, 0], picked[:, 1]


def small_psum(part, tp_size):
    rows, width = part.shape
    blocks = lax.all_to_all(part.reshape(tp_size, rows // tp_size, width), 'tp', 0, 0)
    total = blocks[0]
    for i in range(1, tp_size):
        total = total + blocks[i]
    mine = jnp.broadcast_to(total.astype(jnp.bfloat16)[None], (tp_size, rows // tp_size, width))
    return lax.all_to_all(mine, 'tp', 0, 0).reshape(rows, width)


def swiglu(hidden, gain_vec, w_gu, w_down):
    normed = rms_norm(hidden, gain_vec)
    gate_up = jnp.einsum('...d,kfd->...kf', normed, w_gu, preferred_element_type=jnp.float32)
    gate_val = gate_up[..., 0, :].astype(jnp.bfloat16).astype(jnp.float32)
    up_val = gate_up[..., 1, :].astype(jnp.bfloat16).astype(jnp.float32)
    activated = (jax.nn.silu(gate_val) * up_val).astype(jnp.bfloat16)
    return jnp.einsum('...f,fd->...d', activated, w_down, preferred_element_type=jnp.float32)


def decode_attention(queries, k_tok, v_tok, k_layer, v_layer, visible):
    attn_scale = queries.shape[-1] ** -0.5
    cache_scores = jnp.einsum('bhe,bthe->bht', queries, k_layer, preferred_element_type=jnp.float32) * attn_scale
    cache_scores = jnp.where(visible, cache_scores, MASKED)
    self_score = jnp.einsum('bhe,bhe->bh', queries, k_tok, preferred_element_type=jnp.float32) * attn_scale
    row_max = jnp.maximum(jnp.max(cache_scores, axis=-1), self_score)
    cache_exp = jnp.exp(cache_scores - row_max[..., None])
    self_exp = jnp.exp(self_score - row_max)
    denominator = jnp.sum(cache_exp, axis=-1) + self_exp
    cache_prob = (cache_exp / denominator[..., None]).astype(jnp.bfloat16)
    self_prob = (self_exp / denominator).astype(jnp.bfloat16).astype(jnp.float32)
    context = jnp.einsum('bht,bthe->bhe', cache_prob, v_layer, preferred_element_type=jnp.float32) + self_prob[..., None] * v_tok.astype(jnp.float32)
    return context.astype(jnp.bfloat16)


def run_decode(tokens, k_cache, v_cache, c_len, w_qkv, w_out, w_gu, w_down, gains, tp_size):
    layers, row_count, cache_len, heads_loc, _, head_dim = k_cache.shape
    model_width = tokens.shape[1]
    k_local = k_cache.reshape(layers, row_count, cache_len, heads_loc, head_dim)
    v_local = v_cache.reshape(layers, row_count, cache_len, heads_loc, head_dim)
    wqkv_local = w_qkv.reshape(layers, model_width, 3, heads_loc, head_dim)
    wout_local = w_out.reshape(layers, heads_loc, head_dim, model_width)
    cos_tab, sin_tab = rope_tables(c_len, head_dim)
    cache_pos = jnp.arange(cache_len)
    visible = (cache_pos[None, :] < c_len[:, None])[:, None, :]
    write_at = (cache_pos[None, :] == c_len[:, None])[:, :, None, None]
    k_next = []
    v_next = []
    for layer_idx in range(layers):
        normed = rms_norm(tokens, gains[layer_idx, 0])
        qkv_out = jnp.einsum('bd,dkhe->bkhe', normed, wqkv_local[layer_idx], preferred_element_type=jnp.float32)
        queries = apply_rope(qkv_out[:, 0], cos_tab, sin_tab).astype(jnp.bfloat16)
        k_tok = apply_rope(qkv_out[:, 1], cos_tab, sin_tab).astype(jnp.bfloat16)
        v_tok = qkv_out[:, 2].astype(jnp.bfloat16)
        context = decode_attention(queries, k_tok, v_tok, k_local[layer_idx], v_local[layer_idx], visible)
        part_sum = jnp.einsum('bhe,hed->bd', context, wout_local[layer_idx], preferred_element_type=jnp.float32)
        tokens = add_residual(tokens, small_psum(part_sum, tp_size))
        mlp_part = swiglu(tokens, gains[layer_idx, 1], w_gu[layer_idx], w_down[layer_idx])
        tokens = add_residual(tokens, small_psum(mlp_part, tp_size))
        k_next.append(jnp.where(write_at, k_tok[:, None], k_local[layer_idx]))
        v_next.append(jnp.where(write_at, v_tok[:, None], v_local[layer_idx]))
    return tokens, jnp.stack(k_next).reshape(k_cache.shape), jnp.stack(v_next).reshape(v_cache.shape)


def run_prefill(prompt, s_len, w_qkv, w_out, w_gu, w_down, gains, tp_size, side_size):
    rows, width = prompt.shape
    layers, _, _, heads_loc, head_dim = w_qkv.shape
    me = lax.axis_index('tp')
    right = [(i, (i + 1) % tp_size) for i in range(tp_size)]
    left = [(i, (i - 1) % tp_size) for i in range(tp_size)]
    cos_tab, sin_tab = rope_tables(jnp.arange(rows), head_dim)
    cos_full = jnp.concatenate([cos_tab, cos_tab], axis=-1)
    sin_full = jnp.concatenate([-sin_tab, sin_tab], axis=-1)
    chunk = rows // tp_size
    half = width // 2
    ids = (me + jnp.array([-1, 1, 2, 0], jnp.int32)) % tp_size
    hidden = prompt
    kv_layers = []
    for layer in range(layers):
        shard = heads_loc * head_dim
        w_o = w_out[layer].reshape(shard, width)
        w_t = w_qkv[layer].transpose(1, 2, 0, 3)
        hidden, normed, k, v = front_call(hidden, s_len, gains[layer, 0][None], gains[layer, 1][None], cos_full, sin_full, w_t, w_o, tp_size, side_size)
        kv_layers.append(move_kv(k, v, me, tp_size, side_size))
        a = mlp_call(ids[:2], normed, w_gu[layer], w_down[layer], chunk)
        b = mlp_call(ids[2:], normed, w_gu[layer], w_down[layer], chunk)
        go_r = a[0]
        go_l = a[3]
        for own_r, own_l in ((b[0], b[1]), (a[2], a[1]), (b[2], b[3])):
            go_r = lax.ppermute(go_r, 'tp', right) + own_r
            go_l = lax.ppermute(go_l, 'tp', left) + own_l
        mine = lax.dynamic_slice_in_dim(hidden, me * chunk, chunk, 0)
        down = jnp.concatenate([go_r, go_l], axis=1).astype(jnp.bfloat16)
        hidden = ring_gather(add_residual(mine, down), right, left, me, tp_size)
    return hidden, kv_layers


def solution(mesh):
    tp_size = mesh.shape['tp']
    side_size = mesh.shape['side']
    inst_axes = ('pair', 'side')
    rows_spec = P(inst_axes, None)
    vec_spec = P(inst_axes)
    cache_spec = P(None, inst_axes, None, None, 'tp', None)
    prompt_spec = P(None, inst_axes, None, 'tp', None)
    in_specs = (rows_spec, vec_spec, P(None, None, None, 'tp', None), P(None, 'tp', None, None), P(None, None, 'tp', None), P(None, 'tp', None), P(None, None, None), rows_spec, cache_spec, cache_spec, vec_spec, P(None, None, None, None, 'tp', None), P(None, None, 'tp', None, None), P(None, None, 'tp', None), P(None, 'tp', None), P(None, None, None))
    out_specs = (rows_spec, rows_spec, prompt_spec, prompt_spec, cache_spec, cache_spec)

    def device_fn(prompt_x, s_len, w_qkv_pre, w_out_pre, w_gu_pre, w_down_pre, gain_pre, dec_tokens, k_cache, v_cache, c_len, w_qkv_dec, w_out_dec, w_gu_dec, w_down_dec, gain_dec):
        hidden, kv_layers = run_prefill(prompt_x, s_len, w_qkv_pre, w_out_pre, w_gu_pre, w_down_pre, gain_pre, tp_size, side_size)
        k_prompt = jnp.stack([k for k, _ in kv_layers]).transpose(0, 2, 1, 3)[:, :, :, None, :]
        v_prompt = jnp.stack([v for _, v in kv_layers]).transpose(0, 2, 1, 3)[:, :, :, None, :]
        dec_out, k_cache_new, v_cache_new = run_decode(dec_tokens, k_cache, v_cache, c_len, w_qkv_dec, w_out_dec, w_gu_dec, w_down_dec, gain_dec, tp_size)
        return hidden, dec_out, k_prompt, v_prompt, k_cache_new, v_cache_new

    return jax.shard_map(device_fn, mesh=mesh, in_specs=in_specs, out_specs=out_specs, check_vma=False)
```

```python
import functools

import jax
import jax.numpy as jnp
from jax import lax
from jax.experimental import pallas as pl
from jax.experimental.pallas import tpu as pltpu
from jax.sharding import PartitionSpec as P

EPSILON = 1e-6
THETA = 10000.0
MASKED = -1e30
VMEM_LIMIT = 60 * 1024 * 1024
ANY = pl.BlockSpec(memory_space=pl.ANY)
VM = pl.BlockSpec(memory_space=pltpu.VMEM)
SM = pl.BlockSpec(memory_space=pltpu.SMEM)


def rms_norm(hidden, gain_vec):
    hid_f32 = hidden.astype(jnp.float32)
    inv_rms = lax.rsqrt(jnp.mean(hid_f32 * hid_f32, axis=-1, keepdims=True) + EPSILON)
    return (hid_f32 * inv_rms * gain_vec).astype(jnp.bfloat16)


def add_residual(hidden, update):
    return (hidden.astype(jnp.float32) + update.astype(jnp.float32)).astype(jnp.bfloat16)


def rope_tables(positions, head_dim):
    half_dim = head_dim // 2
    inv_freq = THETA ** (-jnp.arange(half_dim, dtype=jnp.float32) * 2.0 / head_dim)
    angles = positions.astype(jnp.float32)[:, None] * inv_freq[None, :]
    return jnp.cos(angles), jnp.sin(angles)


def front_kernel(len_ref, cos_ref, sin_ref, g1_ref, g2_ref, x_hbm, wqkv_hbm, wo_hbm, h_hbm, n_hbm, k_ref, v_ref, xs, ns, nv, wv, acc, qv, ctx, wo, wsem, xsem, osem, hsem, nsem, ssem, rsem, *, rb, tp_size, side_size):
    n_kind, heads, depth, head_dim = wqkv_hbm.shape
    rows = x_hbm.shape[0]
    n_blk = rows // rb
    shard = heads * head_dim
    width = n_kind * shard
    half = depth // 2
    me = lax.axis_index('tp')
    side = lax.axis_index('side')
    core = lax.rem(side, 2)
    chip = side // 2
    n_chip = side_size // 2
    part = shard // side_size
    tp_of = lambda d: lax.rem(me + d + tp_size, tp_size)
    chip_of = lambda d: lax.rem(chip + d + n_chip, n_chip)
    to_right = {'tp': tp_of(1)}
    to_left = {'tp': tp_of(-1)}
    to_up = {'side': chip_of(1) * 2 + core}
    to_down = {'side': chip_of(-1) * 2 + core}
    to_twin = {'side': chip * 2 + 1 - core}
    whole = pl.ds(0, depth)
    cols_a = pl.ds(0, half)
    cols_b = pl.ds(half, half)

    def send(idx, ref, dev, src=None):
        return pltpu.make_async_remote_copy(src_ref=ref if src is None else src, dst_ref=ref, send_sem=ssem.at[idx], recv_sem=rsem.at[idx], device_id=dev, device_id_type=pl.DeviceIdType.MESH)

    def w_part(d_tp, d_chip, cols, core_id):
        row0 = pl.multiple_of((chip_of(d_chip) * 2 + core_id) * part, 16)
        return wo.at[tp_of(d_tp), pl.ds(row0, part), cols]

    def c_part(d_tp, blk):
        return ctx.at[pl.ds(blk * rb, rb), pl.ds(pl.multiple_of(tp_of(d_tp) * shard, 128), shard)]

    offs = (-1, 1, 2)
    hops = (0, -1, 1, 2)
    sent = []

    def start(copy):
        copy.start()
        sent.append(copy)

    own_slice = wo_hbm.at[pl.ds(pl.multiple_of(side * part, 16), part), :]
    y_send = [
        lambda: send(0, w_part(0, 0, whole, core), to_right, src=own_slice),
        lambda: send(1, w_part(0, 0, whole, core), to_left, src=own_slice),
        lambda: send(2, w_part(-1, 0, cols_a, core), to_right),
        lambda: send(3, w_part(1, 0, cols_b, core), to_left),
    ]
    y_land = [
        lambda: send(0, w_part(-1, 0, whole, core), to_right),
        lambda: send(1, w_part(1, 0, whole, core), to_left),
        lambda: send(2, w_part(-2, 0, cols_a, core), to_right),
        lambda: send(3, w_part(2, 0, cols_b, core), to_left),
    ]

    def x_send(i, kind):
        d = offs[i]
        idx = 4 + 4 * i + kind
        if kind == 0:
            return send(idx, w_part(d, 0, whole, core), to_up)
        if kind == 1:
            return send(idx, w_part(d, 0, whole, core), to_down)
        if kind == 2:
            return send(idx, w_part(d, -1, cols_a, core), to_up)
        return send(idx, w_part(d, 1, cols_b, core), to_down)

    def x_land(i, kind):
        d = offs[i]
        idx = 4 + 4 * i + kind
        if kind == 0:
            return send(idx, w_part(d, -1, whole, core), to_up)
        if kind == 1:
            return send(idx, w_part(d, 1, whole, core), to_down)
        if kind == 2:
            return send(idx, w_part(d, -2, cols_a, core), to_up)
        return send(idx, w_part(d, 2, cols_b, core), to_down)

    def t_send(i, j):
        return send(16 + 4 * i + j, w_part(offs[i], hops[j], whole, core), to_twin)

    def t_land(i, j):
        return send(16 + 4 * i + j, w_part(offs[i], hops[j], whole, 1 - core), to_twin)

    c_right = lambda blk: send(28 + blk, c_part(0, blk), to_right)
    c_left = lambda blk: send(28 + n_blk + blk, c_part(0, blk), to_left)
    c_from_left = lambda blk: send(28 + blk, c_part(-1, blk), to_right)
    c_from_right = lambda blk: send(28 + n_blk + blk, c_part(1, blk), to_left)

    def f_send(blk):
        if blk < n_blk // 2:
            return send(28 + 2 * n_blk + blk, c_part(-1, blk), to_right)
        return send(28 + 2 * n_blk + blk, c_part(1, blk), to_left)

    def f_land(blk):
        return send(28 + 2 * n_blk + blk, c_part(2, blk), to_right if blk < n_blk // 2 else to_left)

    def w_copy(kind, head):
        idx = kind * heads + head
        return pltpu.make_async_copy(wqkv_hbm.at[kind, head], wv.at[:, pl.ds(idx * head_dim, head_dim)], wsem.at[idx])

    x_in = lambda blk: pltpu.make_async_copy(x_hbm.at[pl.ds(blk * rb, rb), :], nv.at[pl.ds(blk * rb, rb), :], xsem.at[blk])
    x_again = lambda blk: pltpu.make_async_copy(x_hbm.at[pl.ds(blk * rb, rb), :], xs.at[blk % 2], xsem.at[n_blk + blk])
    own_w = pltpu.make_async_copy(wo_hbm, wo.at[me], osem.at[0])

    for blk in range(n_blk):
        x_in(blk).start()
    for kind in range(n_kind):
        for head in range(heads):
            w_copy(kind, head).start()
    own_w.start()
    x_again(0).start()
    x_again(1).start()

    barrier = pltpu.get_barrier_semaphore()
    for dev in (to_right, to_left, to_up, to_down, to_twin):
        pl.semaphore_signal(barrier, inc=1, device_id=dev, device_id_type=pl.DeviceIdType.MESH)
    pl.semaphore_wait(barrier, 5)
    start(y_send[0]())
    start(y_send[1]())

    nb = 64
    for blk in range(n_blk):
        x_in(blk).wait()

    def norm_step(i, carry):
        r = pl.ds(pl.multiple_of(i * nb, nb), nb)
        nv[r, :] = rms_norm(nv[r, :], g1_ref[...])
        return carry

    lax.fori_loop(0, rows // nb, norm_step, 0)
    for kind in range(n_kind):
        for head in range(heads):
            w_copy(kind, head).wait()

    def qkv_step(i, carry):
        r = pl.ds(pl.multiple_of(i * rb, rb), rb)
        acc[pl.ds(0, rb), pl.ds(0, width)] = jnp.dot(nv[r, :], wv[...], preferred_element_type=jnp.float32)
        cos_b = cos_ref[r, :]
        sin_b = sin_ref[r, :]
        for head in range(heads):
            for kind, out in ((0, qv), (1, k_ref)):
                idx = (kind * heads + head) * head_dim
                val = acc[0:rb, idx:idx + head_dim]
                out[head, r, :] = (val * cos_b + pltpu.roll(val, head_dim // 2, 1) * sin_b).astype(jnp.bfloat16)
            idx = (2 * heads + head) * head_dim
            v_ref[head, r, :] = acc[0:rb, idx:idx + head_dim].astype(jnp.bfloat16)
        return carry

    lax.fori_loop(0, n_blk // 2, qkv_step, 0)
    for m in range(2):
        y_land[m]().wait_recv()
    for m in range(2):
        start(y_send[2 + m]())
    for i in range(2):
        start(x_send(i, 0))
        start(x_send(i, 1))
        start(t_send(i, 0))
    lax.fori_loop(n_blk // 2, n_blk, qkv_step, 0)
    for m in range(2):
        y_land[2 + m]().wait_recv()
    start(x_send(2, 0))
    start(x_send(2, 1))
    start(t_send(2, 0))

    valid = len_ref[0]
    scale = head_dim ** -0.5
    for blk in range(n_blk):
        span = (blk + 1) * rb
        rowi = lax.broadcasted_iota(jnp.int32, (rb, span), 0) + blk * rb
        coli = lax.broadcasted_iota(jnp.int32, (rb, span), 1)
        seen = (coli <= rowi) & (coli < valid)

        def head_step(head, carry, blk=blk, span=span, seen=seen):
            kk = k_ref[head, pl.ds(0, span), :]
            s = lax.dot_general(qv[head, pl.ds(blk * rb, rb), :], kk, (((1,), (1,)), ((), ())), preferred_element_type=jnp.float32)
            s = jnp.where(seen, s * scale, MASKED)
            p = jnp.exp(s - jnp.max(s, axis=-1, keepdims=True))
            p = (p * (1.0 / jnp.sum(p, axis=-1, keepdims=True))).astype(jnp.bfloat16)
            c = jnp.dot(p, v_ref[head, pl.ds(0, span), :], preferred_element_type=jnp.float32).astype(jnp.bfloat16)
            ctx[pl.ds(blk * rb, rb), pl.ds(pl.multiple_of(me * shard + head * head_dim, head_dim), head_dim)] = c
            return carry

        lax.fori_loop(0, heads, head_step, 0)
        start(c_right(blk))
        start(c_left(blk))

    def relay_x(i):
        for kind in range(2):
            x_land(i, kind).wait_recv()
        for kind in range(2):
            start(x_send(i, 2 + kind))
        start(t_send(i, 1))
        start(t_send(i, 2))

    relay_x(0)
    relay_x(1)
    own_w.wait()

    def add_shard(d, first):
        w_ref = wo.at[tp_of(d)]
        col = pl.ds(pl.multiple_of(tp_of(d) * shard, 128), shard)

        def step(i, carry):
            r = pl.ds(pl.multiple_of(i * rb, rb), rb)
            val = jnp.dot(ctx[r, col], w_ref[...], preferred_element_type=jnp.float32)
            if first:
                acc[r, :] = val
            else:
                acc[r, :] += val
            return carry

        lax.fori_loop(0, n_blk, step, 0)

    for blk in range(n_blk // 2):
        c_from_left(blk).wait_recv()
        start(f_send(blk))
    for blk in range(n_blk // 2, n_blk):
        c_from_right(blk).wait_recv()
        start(f_send(blk))
    add_shard(0, True)
    relay_x(2)
    for i in range(3):
        for kind in range(2, 4):
            x_land(i, kind).wait_recv()
        start(t_send(i, 3))
    for i in range(3):
        for j in range(4):
            t_land(i, j).wait_recv()
    for blk in range(n_blk // 2, n_blk):
        c_from_left(blk).wait_recv()
    for blk in range(n_blk // 2):
        c_from_right(blk).wait_recv()
    add_shard(-1, False)
    add_shard(1, False)

    col = pl.ds(pl.multiple_of(tp_of(2) * shard, 128), shard)
    h_copy = lambda blk: pltpu.make_async_copy(nv.at[pl.ds(blk * rb, rb), :], h_hbm.at[pl.ds(blk * rb, rb), :], hsem.at[blk])
    n_copy = lambda blk: pltpu.make_async_copy(ns.at[blk % 2], n_hbm.at[pl.ds(blk * rb, rb), :], nsem.at[blk])
    w_far = wo.at[tp_of(2)]
    for blk in range(n_blk):
        f_land(blk).wait_recv()
        x_again(blk).wait()
        if blk >= 2:
            n_copy(blk - 2).wait()
        r = pl.ds(blk * rb, rb)
        acc[r, :] += jnp.dot(ctx[r, col], w_far[...], preferred_element_type=jnp.float32)

        def end_step(i, carry, blk=blk):
            r = pl.ds(pl.multiple_of(blk * rb + i * nb, nb), nb)
            q = pl.ds(pl.multiple_of(i * nb, nb), nb)
            h = add_residual(xs[blk % 2, q, :], acc[r, :].astype(jnp.bfloat16))
            nv[r, :] = h
            ns[blk % 2, q, :] = rms_norm(h, g2_ref[...])
            return carry

        lax.fori_loop(0, rb // nb, end_step, 0)
        h_copy(blk).start()
        n_copy(blk).start()
        if blk + 2 < n_blk:
            x_again(blk + 2).start()
    for blk in range(n_blk):
        h_copy(blk).wait()
        if blk >= n_blk - 2:
            n_copy(blk).wait()
    for copy in sent:
        copy.wait_send()


def front_call(x, s_len, gain1, gain2, cos_full, sin_full, w_qkv, w_o, tp_size, side_size):
    rows, depth = x.shape
    n_kind, heads, _, head_dim = w_qkv.shape
    shard = heads * head_dim
    width = n_kind * shard
    rb = 256
    n_blk = rows // rb
    n_msg = 28 + 3 * n_blk
    act = jax.ShapeDtypeStruct((rows, depth), jnp.bfloat16)
    kv = jax.ShapeDtypeStruct((heads, rows, head_dim), jnp.bfloat16)
    dma = pltpu.SemaphoreType.DMA
    return pl.pallas_call(
        functools.partial(front_kernel, rb=rb, tp_size=tp_size, side_size=side_size),
        out_shape=(act, act, kv, kv),
        in_specs=[SM, VM, VM, VM, VM, ANY, ANY, ANY],
        out_specs=(ANY, ANY, VM, VM),
        scratch_shapes=[
            pltpu.VMEM((2, rb, depth), jnp.bfloat16),
            pltpu.VMEM((2, rb, depth), jnp.bfloat16),
            pltpu.VMEM((rows, depth), jnp.bfloat16),
            pltpu.VMEM((depth, width), jnp.bfloat16),
            pltpu.VMEM((rows, depth), jnp.float32),
            pltpu.VMEM((heads, rows, head_dim), jnp.bfloat16),
            pltpu.VMEM((rows, tp_size * shard), jnp.bfloat16),
            pltpu.VMEM((tp_size, shard, depth), jnp.bfloat16),
            dma((n_kind * heads,)), dma((2 * n_blk,)), dma((1,)), dma((n_blk,)), dma((n_blk,)), dma((n_msg,)), dma((n_msg,)),
        ],
        compiler_params=pltpu.CompilerParams(vmem_limit_bytes=67043328, collective_id=0, has_side_effects=True),
        cost_estimate=pl.CostEstimate(flops=2 * rows * depth * (width + tp_size * shard), bytes_accessed=2 * (4 * rows * depth + depth * width), transcendentals=0),
        name="front",
    )(s_len, cos_full, sin_full, gain1, gain2, x, w_qkv, w_o)


def back_kernel(h_hbm, n_hbm, wgu_hbm, wd_hbm, k_hbm, v_hbm, tok_ref, len_ref, dcos_ref, dsin_ref, dg1_ref, dg2_ref, wqd_hbm, wod_hbm, wgud_hbm, wdd_hbm, kc_hbm, vc_hbm, out_hbm, kp_hbm, vp_hbm, dec_ref, ktok_ref, vtok_ref, nv, act, gu_v, wd_v, part, land, hb, hres, cbuf, dscr, dq, dprob, dctx, dpart, dland, dtok, dact, nsem, gsem, dsem, hsem, osem, qsem, dgsem, csem, ssem, rsem, *, fb, tp_size, side_size):
    ff, depth = wd_hbm.shape
    heads, rows, head_dim = k_hbm.shape
    chunk = rows // tp_size
    half = depth // 2
    sub = half // 2
    me = lax.axis_index('tp')
    side = lax.axis_index('side')
    tp_of = lambda d: lax.rem(me + d + tp_size, tp_size)
    to_right = {'tp': tp_of(1)}
    to_left = {'tp': tp_of(-1)}
    mate = lax.rem(side + side_size // 2, side_size)
    order = (-1, 1, 2, 0)
    pieces = [(f, min(fb, ff - f)) for f in range(0, ff, fb)]
    sent = []

    def start(copy):
        copy.start()
        sent.append(copy)

    def remote(idx, src, dst, dev):
        return pltpu.make_async_remote_copy(src_ref=src, dst_ref=dst, send_sem=ssem.at[idx], recv_sem=rsem.at[idx], device_id=dev, device_id_type=pl.DeviceIdType.MESH)

    def rows_of(d):
        return pl.ds(pl.multiple_of(tp_of(d) * chunk, chunk), chunk)

    def n_copy(c):
        return pltpu.make_async_copy(n_hbm.at[rows_of(order[c]), :], nv.at[pl.ds(c * chunk, chunk), :], nsem.at[c])

    def gu_copy(p, which):
        f, size = pieces[p]
        return pltpu.make_async_copy(wgu_hbm.at[which, pl.ds(f, size), :], gu_v.at[which, pl.ds(f, size), :], gsem.at[2 * p + which])

    wd_copy = pltpu.make_async_copy(wd_hbm, wd_v, dsem.at[0])
    h_copy = pltpu.make_async_copy(h_hbm.at[rows_of(0), :], hres, hsem.at[0])

    n_copy(0).start()
    n_copy(1).start()
    ahead = 3
    for p in range(ahead):
        gu_copy(p, 0).start()
        gu_copy(p, 1).start()

    barrier = pltpu.get_barrier_semaphore()
    peers = [{'tp': tp_of(d)} for d in range(1, tp_size)] + [{'tp': t, 'side': mate} for t in range(tp_size)]
    for dev in peers:
        pl.semaphore_signal(barrier, inc=1, device_id=dev, device_id_type=pl.DeviceIdType.MESH)
    pl.semaphore_wait(barrier, len(peers))

    def kv_send(i, src, dst, idx):
        head = me * heads + i
        return remote(idx, src.at[i], dst.at[head // tp_size], {'tp': lax.rem(head, tp_size), 'side': mate})

    def kv_land(i, src, dst, idx):
        slot = lax.rem(me - i + heads, heads)
        return remote(idx, src.at[i], dst.at[slot], {'tp': me, 'side': mate})

    for i in range(heads):
        start(kv_send(i, k_hbm, kp_hbm, i))
        start(kv_send(i, v_hbm, vp_hbm, heads + i))
    base = 2 * heads

    nt = (((1,), (1,)), ((), ()))
    span = 2 * chunk

    def gate_up(c, f, size):
        n_rows = nv[c * chunk:c * chunk + span, :]
        gate = lax.dot_general(n_rows, gu_v[0, f:f + size, :], nt, preferred_element_type=jnp.float32)
        up = lax.dot_general(n_rows, gu_v[1, f:f + size, :], nt, preferred_element_type=jnp.float32)
        gate = gate.astype(jnp.bfloat16).astype(jnp.float32)
        up = up.astype(jnp.bfloat16).astype(jnp.float32)
        act[:, f:f + size] = (gate * jax.nn.sigmoid(gate) * up).astype(jnp.bfloat16)

    def down(c, row, n_rows, lo):
        for col in range(lo, lo + half, fb):
            part[(c + row) * chunk:(c + row) * chunk + n_rows, col:col + fb] = jnp.dot(act[row * chunk:row * chunk + n_rows, :], wd_v[:, col:col + fb], preferred_element_type=jnp.float32)

    n_copy(0).wait()
    n_copy(1).wait()
    for p, (f, size) in enumerate(pieces):
        gu_copy(p, 0).wait()
        gu_copy(p, 1).wait()
        if p + ahead < len(pieces):
            gu_copy(p + ahead, 0).start()
            gu_copy(p + ahead, 1).start()
        if p + ahead == len(pieces):
            wd_copy.start()
            n_copy(2).start()
            n_copy(3).start()
            h_copy.start()
        gate_up(0, f, size)
    wd_copy.wait()

    cols = lambda way, q: pl.ds(way * half + q * sub, sub)
    devs = (to_right, to_left)

    def rs(step, way, q):
        idx = base + 4 * step + 2 * way + q
        dst = land.at[step, :, cols(way, q)]
        if step == 0:
            src = part.at[pl.ds(way * chunk, chunk), cols(way, q)]
        else:
            src = land.at[step - 1, :, cols(way, q)]
        return remote(idx, src, dst, devs[way])

    down(0, 0, chunk, 0)
    start(rs(0, 0, 0))
    start(rs(0, 0, 1))
    down(0, 1, chunk, half)
    start(rs(0, 1, 0))
    start(rs(0, 1, 1))
    down(0, 0, chunk, half)
    down(0, 1, chunk, 0)
    n_copy(2).wait()
    n_copy(3).wait()
    for f, size in pieces:
        gate_up(2, f, size)
    d_rows = tok_ref.shape[0]
    d_heads = heads
    shard = heads * head_dim
    n_kind = wqd_hbm.shape[0]
    cache_len = kc_hbm.shape[2]
    k_half = depth // 2
    lo_rows = 3 * head_dim

    def wq_copy(kind, head, hv):
        idx = kind * d_heads + head
        return pltpu.make_async_copy(wqd_hbm.at[kind, head, pl.ds(hv * k_half, k_half), :], gu_v.at[hv, pl.ds(0, k_half), pl.ds(idx * head_dim, head_dim)], qsem.at[2 * idx + hv])

    wo_lo = pltpu.make_async_copy(wod_hbm.at[pl.ds(0, lo_rows), :], gu_v.at[0, pl.ds(k_half, lo_rows), :], dsem.at[1])
    wo_hi = pltpu.make_async_copy(wod_hbm.at[pl.ds(lo_rows, shard - lo_rows), :], gu_v.at[1, pl.ds(k_half, shard - lo_rows), :], dsem.at[2])
    wdd_copy = pltpu.make_async_copy(wdd_hbm, wd_v, dsem.at[3])

    def gud_copy(p, which):
        f, size = pieces[p]
        return pltpu.make_async_copy(wgud_hbm.at[which, pl.ds(f, size), :], gu_v.at[which, pl.ds(f, size), :], dgsem.at[2 * p + which])

    def c_copy(src, b, slot):
        return pltpu.make_async_copy(src.at[b], cbuf.at[slot], csem.at[slot])

    for kind in range(n_kind):
        for head in range(d_heads):
            for hv in range(2):
                wq_copy(kind, head, hv).start()
    wo_lo.start()
    wo_hi.start()
    c_copy(kc_hbm, 0, 0).start()
    down(2, 0, span, 0)
    down(2, 0, span, half)
    wdd_copy.start()

    nb = 64
    slots = ((2, 2), (1, 0), (3, 3))

    def event(step, q):
        for way in range(2):
            rs(step, way, q).wait_recv()

            def add_step(i, carry, way=way):
                r = pl.ds(pl.multiple_of(i * nb, nb), nb)
                pr = pl.ds(pl.multiple_of(slots[step][way] * chunk + i * nb, nb), nb)
                land[step, r, cols(way, q)] += part[pr, cols(way, q)]
                return carry

            lax.fori_loop(0, chunk // nb, add_step, 0)
            start(rs(step + 1, way, q))

    def decode_qkv():
        normed = rms_norm(tok_ref[...], dg1_ref[...])
        for kind in range(n_kind):
            for head in range(d_heads):
                for hv in range(2):
                    wq_copy(kind, head, hv).wait()
        cos_b = dcos_ref[...]
        sin_b = dsin_ref[...]
        for kind in range(n_kind):
            c0 = kind * shard
            val = jnp.dot(normed[:, :k_half], gu_v[0, 0:k_half, c0:c0 + shard], preferred_element_type=jnp.float32)
            val += jnp.dot(normed[:, k_half:], gu_v[1, 0:k_half, c0:c0 + shard], preferred_element_type=jnp.float32)
            for head in range(d_heads):
                one = val[:, head * head_dim:(head + 1) * head_dim]
                if kind < 2:
                    one = one * cos_b + pltpu.roll(one, head_dim // 2, 1) * sin_b
                (dq, ktok_ref, vtok_ref)[kind][head] = one.astype(jnp.bfloat16)

    row_id = lax.broadcasted_iota(jnp.int32, (d_rows, 1), 0)

    def over_rows(src, body):
        def step(b, carry):
            slot = lax.rem(b, 2)
            c_copy(src, b, slot).wait()

            @pl.when(b + 1 < d_rows)
            def _():
                c_copy(src, b + 1, 1 - slot).start()

            body(b, slot)
            return carry

        lax.fori_loop(0, d_rows, step, 0)

    def decode_scores():
        def body(b, slot):
            for head in range(d_heads):
                sc = lax.dot_general(dq[head], cbuf[slot, head], nt, preferred_element_type=jnp.float32)
                dscr[head] = jnp.where(row_id == b, sc, dscr[head])

        over_rows(kc_hbm, body)
        c_copy(vc_hbm, 0, 0).start()
        scale = head_dim ** -0.5
        pos = lax.broadcasted_iota(jnp.int32, (d_rows, cache_len), 1)
        seen = pos < len_ref[...]
        for head in range(d_heads):
            sc = jnp.where(seen, dscr[head] * scale, MASKED)
            own_sc = jnp.sum(dq[head].astype(jnp.float32) * ktok_ref[head].astype(jnp.float32), axis=-1, keepdims=True) * scale
            top = jnp.maximum(jnp.max(sc, axis=-1, keepdims=True), own_sc)
            ex = jnp.exp(sc - top)
            own_ex = jnp.exp(own_sc - top)
            den = jnp.sum(ex, axis=-1, keepdims=True) + own_ex
            dprob[head] = (ex / den).astype(jnp.bfloat16)
            own_p = (own_ex / den).astype(jnp.bfloat16).astype(jnp.float32)
            dctx[:, head * head_dim:(head + 1) * head_dim] = own_p * vtok_ref[head].astype(jnp.float32)

    def decode_context():
        def body(b, slot):
            for head in range(d_heads):
                got = jnp.dot(dprob[head], cbuf[slot, head], preferred_element_type=jnp.float32)
                hc = slice(head * head_dim, (head + 1) * head_dim)
                dctx[:, hc] += jnp.where(row_id == b, got, 0.0)

        over_rows(vc_hbm, body)
        wo_lo.wait()
        wo_hi.wait()
        ctx_b = dctx[...].astype(jnp.bfloat16)
        val = jnp.dot(ctx_b[:, :lo_rows], gu_v[0, k_half:k_half + lo_rows, :], preferred_element_type=jnp.float32)
        dpart[0] = val + jnp.dot(ctx_b[:, lo_rows:], gu_v[1, k_half:k_half + shard - lo_rows, :], preferred_element_type=jnp.float32)
        for p in range(len(pieces)):
            gud_copy(p, 0).start()
            gud_copy(p, 1).start()

    base_d = base + 24
    d_cols = lambda d: pl.ds(pl.multiple_of(tp_of(d) * shard, 128), shard)

    def d_scatter(n, d):
        return remote(base_d + 6 * n + d - 1, dpart.at[n, :, d_cols(d)], dland.at[n, d - 1], {'tp': tp_of(d)})

    def d_gather(n, d):
        return remote(base_d + 6 * n + 2 + d, dtok.at[n, :, d_cols(0)], dtok.at[n, :, d_cols(0)], {'tp': tp_of(d)})

    def d_gather_land(n, d):
        return remote(base_d + 6 * n + 2 + d, dtok.at[n, :, d_cols(-d)], dtok.at[n, :, d_cols(-d)], {'tp': tp_of(d)})

    def decode_scatter(n):
        for d in range(1, tp_size):
            start(d_scatter(n, d))

    def decode_sum(n, before):
        for d in range(1, tp_size):
            d_scatter(n, d).wait_recv()
        total = dpart[n, :, d_cols(0)]
        for d in range(1, tp_size):
            total = total + dland[n, d - 1]
        dtok[n, :, d_cols(0)] = add_residual(before[:, d_cols(0)], total.astype(jnp.bfloat16))
        for d in range(1, tp_size):
            start(d_gather(n, d))

    def decode_gathered(n):
        for d in range(1, tp_size):
            d_gather_land(n, d).wait_recv()

    def decode_gate_up():
        normed = rms_norm(dtok[0], dg2_ref[...])
        for p, (f, size) in enumerate(pieces):
            gud_copy(p, 0).wait()
            gud_copy(p, 1).wait()
            gate = lax.dot_general(normed, gu_v[0, f:f + size, :], nt, preferred_element_type=jnp.float32)
            up = lax.dot_general(normed, gu_v[1, f:f + size, :], nt, preferred_element_type=jnp.float32)
            gate = gate.astype(jnp.bfloat16).astype(jnp.float32)
            up = up.astype(jnp.bfloat16).astype(jnp.float32)
            dact[:, f:f + size] = (gate * jax.nn.sigmoid(gate) * up).astype(jnp.bfloat16)

    def decode_down():
        wdd_copy.wait()
        dpart[1] = jnp.dot(dact[...], wd_v[...], preferred_element_type=jnp.float32)

    event(0, 0)
    decode_qkv()
    event(0, 1)
    decode_scores()
    decode_context()
    decode_scatter(0)
    event(1, 0)
    decode_sum(0, tok_ref)
    event(1, 1)
    decode_gathered(0)
    decode_gate_up()
    decode_down()
    decode_scatter(1)

    base_ag = base + 12
    h_copy.wait()

    def ag(way, q, dev_i):
        idx = base_ag + 4 * way + 2 * q + dev_i
        return remote(idx, hb.at[:, cols(way, q)], out_hbm.at[rows_of(0), cols(way, q)], devs[dev_i])

    def ag_land(way, q, dev_i):
        idx = base_ag + 4 * way + 2 * q + dev_i
        return remote(idx, hb.at[:, cols(way, q)], out_hbm.at[rows_of(-1 if dev_i == 0 else 1), cols(way, q)], devs[dev_i])

    def fwd(way, q):
        ref = out_hbm.at[rows_of(-1 if way == 0 else 1), cols(way, q)]
        return remote(base_ag + 8 + 2 * way + q, ref, ref, devs[way])

    def fwd_land(way, q):
        ref = out_hbm.at[rows_of(2), cols(way, q)]
        return remote(base_ag + 8 + 2 * way + q, ref, ref, devs[way])

    for q in range(2):
        for way in range(2):
            rs(2, way, q).wait_recv()

            def end_step(i, carry, way=way, q=q):
                r = pl.ds(pl.multiple_of(i * nb, nb), nb)
                pr = pl.ds(pl.multiple_of(3 * chunk + i * nb, nb), nb)
                total = land[2, r, cols(way, q)] + part[pr, cols(way, q)]
                hb[r, cols(way, q)] = add_residual(hres[r, cols(way, q)], total.astype(jnp.bfloat16))
                return carry

            lax.fori_loop(0, chunk // nb, end_step, 0)
            start(ag(way, q, way))
            start(ag(way, q, 1 - way))
        if q == 0:
            decode_sum(1, dtok.at[0])
    own = pltpu.make_async_copy(hb, out_hbm.at[rows_of(0), :], osem.at[0])
    own.start()
    for q in range(2):
        for way in range(2):
            ag_land(way, q, way).wait_recv()
            start(fwd(way, q))
    for q in range(2):
        for way in range(2):
            ag_land(way, q, 1 - way).wait_recv()
    for i in range(heads):
        kv_land(i, k_hbm, kp_hbm, i).wait_recv()
        kv_land(i, v_hbm, vp_hbm, heads + i).wait_recv()
    for q in range(2):
        for way in range(2):
            fwd_land(way, q).wait_recv()
    own.wait()
    decode_gathered(1)
    dec_ref[...] = dtok[1]
    for copy in sent:
        copy.wait_send()


def back_call(h, normed, w_gu, w_down, k, v, dec, tp_size, side_size):
    rows, depth = h.shape
    ff = w_down.shape[0]
    heads = k.shape[0]
    chunk = rows // tp_size
    fb = 256
    n_piece = -(-ff // fb)
    n_msg = 2 * heads + 12 + 12 + 12
    d_rows = dec[0].shape[0]
    head_dim = k.shape[2]
    cache_len = dec[10].shape[2]
    dma = pltpu.SemaphoreType.DMA
    bf16 = jnp.bfloat16
    kv = jax.ShapeDtypeStruct(k.shape, bf16)
    return pl.pallas_call(
        functools.partial(back_kernel, fb=fb, tp_size=tp_size, side_size=side_size),
        out_shape=(jax.ShapeDtypeStruct((rows, depth), bf16), kv, kv, jax.ShapeDtypeStruct((d_rows, depth), bf16)) + (jax.ShapeDtypeStruct((heads, d_rows, head_dim), bf16),) * 2,
        in_specs=[ANY] * 6 + [VM] * 6 + [ANY] * 6,
        out_specs=(ANY,) * 3 + (VM,) * 3,
        scratch_shapes=[
            pltpu.VMEM((rows, depth), bf16),
            pltpu.VMEM((2 * chunk, ff), bf16),
            pltpu.VMEM((2, ff, depth), bf16),
            pltpu.VMEM((ff, depth), bf16),
            pltpu.VMEM((rows, depth), jnp.float32),
            pltpu.VMEM((3, chunk, depth), jnp.float32),
            pltpu.VMEM((chunk, depth), bf16),
            pltpu.VMEM((chunk, depth), bf16),
            pltpu.VMEM((2, heads, cache_len, head_dim), bf16),
            pltpu.VMEM((heads, d_rows, cache_len), jnp.float32),
            pltpu.VMEM((heads, d_rows, head_dim), bf16),
            pltpu.VMEM((heads, d_rows, cache_len), bf16),
            pltpu.VMEM((d_rows, heads * head_dim), jnp.float32),
            pltpu.VMEM((2, d_rows, depth), jnp.float32),
            pltpu.VMEM((2, tp_size - 1, d_rows, heads * head_dim), jnp.float32),
            pltpu.VMEM((2, d_rows, depth), bf16),
            pltpu.VMEM((d_rows, ff), bf16),
            dma((tp_size,)), dma((2 * n_piece,)), dma((4,)), dma((1,)), dma((1,)), dma((6 * heads,)), dma((2 * n_piece,)), dma((2,)), dma((n_msg,)), dma((n_msg,)),
        ],
        compiler_params=pltpu.CompilerParams(vmem_limit_bytes=67043328, collective_id=1, has_side_effects=True),
        cost_estimate=pl.CostEstimate(flops=6 * rows * ff * depth, bytes_accessed=6 * ff * depth + 8 * rows * depth, transcendentals=0),
        name="back",
    )(h, normed, w_gu, w_down, k, v, *dec)


def write_cache(cache, new, at):
    row_count, cache_len = cache.shape[:2]
    here = (jnp.arange(cache_len)[None, :] == at[:, None])[:, :, None, None, None]
    return jnp.where(here, new.transpose(1, 0, 2)[:, None, :, None, :], cache)


def run_layers(prompt, s_len, pre, tokens, k_cache, v_cache, c_len, dec, tp_size, side_size):
    w_qkv, w_out, w_gu, w_down, gains = pre
    dw_qkv, dw_out, dw_gu, dw_down, dgains = dec
    rows, width = prompt.shape
    layers, _, _, heads_loc, head_dim = w_qkv.shape
    shard = heads_loc * head_dim
    d_rows, cache_len = k_cache.shape[1:3]

    def full_tables(positions):
        cos_tab, sin_tab = rope_tables(positions, head_dim)
        return jnp.concatenate([cos_tab, cos_tab], axis=-1), jnp.concatenate([-sin_tab, sin_tab], axis=-1)

    cos_full, sin_full = full_tables(jnp.arange(rows))
    d_cos, d_sin = full_tables(c_len)
    hidden = prompt
    outs = []
    for layer in range(layers):
        w_t = w_qkv[layer].transpose(1, 2, 0, 3)
        hidden, normed, k, v = front_call(hidden, s_len, gains[layer, 0][None], gains[layer, 1][None], cos_full, sin_full, w_t, w_out[layer].reshape(shard, width), tp_size, side_size)
        by_head = lambda cache: cache[layer].reshape(d_rows, cache_len, heads_loc, head_dim).transpose(0, 2, 1, 3)
        dec_args = (tokens, c_len[:, None], d_cos, d_sin, dgains[layer, 0][None], dgains[layer, 1][None], dw_qkv[layer].reshape(width, 3, heads_loc, head_dim).transpose(1, 2, 0, 3), dw_out[layer].reshape(shard, width), dw_gu[layer], dw_down[layer], by_head(k_cache), by_head(v_cache))
        hidden, k_inst, v_inst, tokens, k_tok, v_tok = back_call(hidden, normed, w_gu[layer], w_down[layer], k, v, dec_args, tp_size, side_size)
        outs.append((k_inst.transpose(1, 0, 2)[:, :, None, :], v_inst.transpose(1, 0, 2)[:, :, None, :], write_cache(k_cache[layer], k_tok, c_len), write_cache(v_cache[layer], v_tok, c_len)))
    return (hidden, tokens) + tuple(jnp.stack(parts) for parts in zip(*outs))


def solution(mesh):
    tp_size = mesh.shape['tp']
    side_size = mesh.shape['side']
    inst_axes = ('pair', 'side')
    rows_spec = P(inst_axes, None)
    vec_spec = P(inst_axes)
    cache_spec = P(None, inst_axes, None, None, 'tp', None)
    prompt_spec = P(None, inst_axes, None, 'tp', None)
    in_specs = (rows_spec, vec_spec, P(None, None, None, 'tp', None), P(None, 'tp', None, None), P(None, None, 'tp', None), P(None, 'tp', None), P(None, None, None), rows_spec, cache_spec, cache_spec, vec_spec, P(None, None, None, None, 'tp', None), P(None, None, 'tp', None, None), P(None, None, 'tp', None), P(None, 'tp', None), P(None, None, None))
    out_specs = (rows_spec, rows_spec, prompt_spec, prompt_spec, cache_spec, cache_spec)

    def device_fn(prompt_x, s_len, w_qkv_pre, w_out_pre, w_gu_pre, w_down_pre, gain_pre, dec_tokens, k_cache, v_cache, c_len, w_qkv_dec, w_out_dec, w_gu_dec, w_down_dec, gain_dec):
        pre = (w_qkv_pre, w_out_pre, w_gu_pre, w_down_pre, gain_pre)
        dec = (w_qkv_dec, w_out_dec, w_gu_dec, w_down_dec, gain_dec)
        return run_layers(prompt_x, s_len, pre, dec_tokens, k_cache, v_cache, c_len, dec, tp_size, side_size)

    return jax.shard_map(device_fn, mesh=mesh, in_specs=in_specs, out_specs=out_specs, check_vma=False)
```

```python
import functools

import jax
import jax.numpy as jnp
from jax import lax
from jax.experimental import pallas as pl
from jax.experimental.pallas import tpu as pltpu
from jax.sharding import PartitionSpec as P

EPSILON = 1e-6
THETA = 10000.0
MASKED = -1e30
VMEM_LIMIT = 60 * 1024 * 1024
ANY = pl.BlockSpec(memory_space=pl.ANY)
VM = pl.BlockSpec(memory_space=pltpu.VMEM)
SM = pl.BlockSpec(memory_space=pltpu.SMEM)


def rms_norm(hidden, gain_vec):
    hid_f32 = hidden.astype(jnp.float32)
    inv_rms = lax.rsqrt(jnp.mean(hid_f32 * hid_f32, axis=-1, keepdims=True) + EPSILON)
    return (hid_f32 * inv_rms * gain_vec).astype(jnp.bfloat16)


def add_residual(hidden, update):
    return (hidden.astype(jnp.float32) + update.astype(jnp.float32)).astype(jnp.bfloat16)


def rope_tables(positions, head_dim):
    half_dim = head_dim // 2
    inv_freq = THETA ** (-jnp.arange(half_dim, dtype=jnp.float32) * 2.0 / head_dim)
    angles = positions.astype(jnp.float32)[:, None] * inv_freq[None, :]
    return jnp.cos(angles), jnp.sin(angles)


def front_kernel(len_ref, cos_ref, sin_ref, g_ref, x_hbm, wqkv_hbm, wo_hbm, h_hbm, n_hbm, k_ref, v_ref, xs, ns, nv, wv, acc, qv, ctx, wo, wsem, xsem, osem, hsem, nsem, ssem, rsem, *, rb, tp_size, side_size):
    n_kind, heads, depth, head_dim = wqkv_hbm.shape
    rows = x_hbm.shape[0]
    n_blk = rows // rb
    shard = heads * head_dim
    width = n_kind * shard
    half = depth // 2
    me = lax.axis_index('tp')
    side = lax.axis_index('side')
    core = lax.rem(side, 2)
    chip = side // 2
    n_chip = side_size // 2
    part = shard // side_size
    tp_of = lambda d: lax.rem(me + d + tp_size, tp_size)
    chip_of = lambda d: lax.rem(chip + d + n_chip, n_chip)
    to_right = {'tp': tp_of(1)}
    to_left = {'tp': tp_of(-1)}
    to_up = {'side': chip_of(1) * 2 + core}
    to_down = {'side': chip_of(-1) * 2 + core}
    to_twin = {'side': chip * 2 + 1 - core}
    whole = pl.ds(0, depth)
    cols_a = pl.ds(0, half)
    cols_b = pl.ds(half, half)

    def send(idx, ref, dev, src=None):
        return pltpu.make_async_remote_copy(src_ref=ref if src is None else src, dst_ref=ref, send_sem=ssem.at[idx], recv_sem=rsem.at[idx], device_id=dev, device_id_type=pl.DeviceIdType.MESH)

    def w_part(d_tp, d_chip, cols, core_id):
        row0 = pl.multiple_of((chip_of(d_chip) * 2 + core_id) * part, 16)
        return wo.at[tp_of(d_tp), pl.ds(row0, part), cols]

    def c_part(d_tp, blk):
        return ctx.at[pl.ds(blk * rb, rb), pl.ds(pl.multiple_of(tp_of(d_tp) * shard, 128), shard)]

    offs = (-1, 1, 2)
    hops = (0, -1, 1, 2)
    sent = []

    def start(copy):
        copy.start()
        sent.append(copy)

    own_slice = wo_hbm.at[pl.ds(pl.multiple_of(side * part, 16), part), :]
    y_send = [
        lambda: send(0, w_part(0, 0, whole, core), to_right, src=own_slice),
        lambda: send(1, w_part(0, 0, whole, core), to_left, src=own_slice),
        lambda: send(2, w_part(-1, 0, cols_a, core), to_right),
        lambda: send(3, w_part(1, 0, cols_b, core), to_left),
    ]
    y_land = [
        lambda: send(0, w_part(-1, 0, whole, core), to_right),
        lambda: send(1, w_part(1, 0, whole, core), to_left),
        lambda: send(2, w_part(-2, 0, cols_a, core), to_right),
        lambda: send(3, w_part(2, 0, cols_b, core), to_left),
    ]

    def x_send(i, kind):
        d = offs[i]
        idx = 4 + 4 * i + kind
        if kind == 0:
            return send(idx, w_part(d, 0, whole, core), to_up)
        if kind == 1:
            return send(idx, w_part(d, 0, whole, core), to_down)
        if kind == 2:
            return send(idx, w_part(d, -1, cols_a, core), to_up)
        return send(idx, w_part(d, 1, cols_b, core), to_down)

    def x_land(i, kind):
        d = offs[i]
        idx = 4 + 4 * i + kind
        if kind == 0:
            return send(idx, w_part(d, -1, whole, core), to_up)
        if kind == 1:
            return send(idx, w_part(d, 1, whole, core), to_down)
        if kind == 2:
            return send(idx, w_part(d, -2, cols_a, core), to_up)
        return send(idx, w_part(d, 2, cols_b, core), to_down)

    def t_send(i, j):
        return send(16 + 4 * i + j, w_part(offs[i], hops[j], whole, core), to_twin)

    def t_land(i, j):
        return send(16 + 4 * i + j, w_part(offs[i], hops[j], whole, 1 - core), to_twin)

    c_right = lambda blk: send(28 + blk, c_part(0, blk), to_right)
    c_left = lambda blk: send(28 + n_blk + blk, c_part(0, blk), to_left)
    c_from_left = lambda blk: send(28 + blk, c_part(-1, blk), to_right)
    c_from_right = lambda blk: send(28 + n_blk + blk, c_part(1, blk), to_left)

    def f_send(blk):
        if blk < n_blk // 2:
            return send(28 + 2 * n_blk + blk, c_part(-1, blk), to_right)
        return send(28 + 2 * n_blk + blk, c_part(1, blk), to_left)

    def f_land(blk):
        return send(28 + 2 * n_blk + blk, c_part(2, blk), to_right if blk < n_blk // 2 else to_left)

    def w_copy(kind, head):
        idx = kind * heads + head
        return pltpu.make_async_copy(wqkv_hbm.at[kind, head], wv.at[:, pl.ds(idx * head_dim, head_dim)], wsem.at[idx])

    x_in = lambda blk: pltpu.make_async_copy(x_hbm.at[pl.ds(blk * rb, rb), :], nv.at[pl.ds(blk * rb, rb), :], xsem.at[blk])
    x_again = lambda blk: pltpu.make_async_copy(x_hbm.at[pl.ds(blk * rb, rb), :], xs.at[blk % 2], xsem.at[n_blk + blk])
    own_w = pltpu.make_async_copy(wo_hbm, wo.at[me], osem.at[0])

    for blk in range(n_blk):
        x_in(blk).start()
    for kind in range(n_kind):
        for head in range(heads):
            w_copy(kind, head).start()
    own_w.start()
    x_again(0).start()
    x_again(1).start()

    barrier = pltpu.get_barrier_semaphore()
    for dev in (to_right, to_left, to_up, to_down, to_twin):
        pl.semaphore_signal(barrier, inc=1, device_id=dev, device_id_type=pl.DeviceIdType.MESH)
    pl.semaphore_wait(barrier, 5)
    start(y_send[0]())
    start(y_send[1]())

    nb = 64
    for blk in range(n_blk):
        x_in(blk).wait()

    def norm_step(i, carry):
        r = pl.ds(pl.multiple_of(i * nb, nb), nb)
        nv[r, :] = rms_norm(nv[r, :], g_ref[0:1, :])
        return carry

    lax.fori_loop(0, rows // nb, norm_step, 0)
    for kind in range(n_kind):
        for head in range(heads):
            w_copy(kind, head).wait()

    def qkv_step(i, carry):
        r = pl.ds(pl.multiple_of(i * rb, rb), rb)
        acc[pl.ds(0, rb), pl.ds(0, width)] = jnp.dot(nv[r, :], wv[...], preferred_element_type=jnp.float32)
        cos_b = cos_ref[r, :]
        sin_b = sin_ref[r, :]
        for head in range(heads):
            for kind, out in ((0, qv), (1, k_ref)):
                idx = (kind * heads + head) * head_dim
                val = acc[0:rb, idx:idx + head_dim]
                out[head, r, :] = (val * cos_b + pltpu.roll(val, head_dim // 2, 1) * sin_b).astype(jnp.bfloat16)
            idx = (2 * heads + head) * head_dim
            v_ref[head, r, :] = acc[0:rb, idx:idx + head_dim].astype(jnp.bfloat16)
        return carry

    lax.fori_loop(0, n_blk // 2, qkv_step, 0)
    for m in range(2):
        y_land[m]().wait_recv()
    for m in range(2):
        start(y_send[2 + m]())
    for i in range(2):
        start(x_send(i, 0))
        start(x_send(i, 1))
        start(t_send(i, 0))
    lax.fori_loop(n_blk // 2, n_blk, qkv_step, 0)
    for m in range(2):
        y_land[2 + m]().wait_recv()
    start(x_send(2, 0))
    start(x_send(2, 1))
    start(t_send(2, 0))

    valid = len_ref[0]
    scale = head_dim ** -0.5
    for blk in range(n_blk):
        span = (blk + 1) * rb
        rowi = lax.broadcasted_iota(jnp.int32, (rb, span), 0) + blk * rb
        coli = lax.broadcasted_iota(jnp.int32, (rb, span), 1)
        seen = (coli <= rowi) & (coli < valid)

        def head_step(head, carry, blk=blk, span=span, seen=seen):
            kk = k_ref[head, pl.ds(0, span), :]
            s = lax.dot_general(qv[head, pl.ds(blk * rb, rb), :], kk, (((1,), (1,)), ((), ())), preferred_element_type=jnp.float32)
            s = jnp.where(seen, s * scale, MASKED)
            p = jnp.exp(s - jnp.max(s, axis=-1, keepdims=True))
            p = (p * (1.0 / jnp.sum(p, axis=-1, keepdims=True))).astype(jnp.bfloat16)
            c = jnp.dot(p, v_ref[head, pl.ds(0, span), :], preferred_element_type=jnp.float32).astype(jnp.bfloat16)
            ctx[pl.ds(blk * rb, rb), pl.ds(pl.multiple_of(me * shard + head * head_dim, head_dim), head_dim)] = c
            return carry

        lax.fori_loop(0, heads, head_step, 0)
        start(c_right(blk))
        start(c_left(blk))

    def relay_x(i):
        for kind in range(2):
            x_land(i, kind).wait_recv()
        for kind in range(2):
            start(x_send(i, 2 + kind))
        start(t_send(i, 1))
        start(t_send(i, 2))

    relay_x(0)
    relay_x(1)
    own_w.wait()

    def add_shard(d, first):
        w_ref = wo.at[tp_of(d)]
        col = pl.ds(pl.multiple_of(tp_of(d) * shard, 128), shard)

        def step(i, carry):
            r = pl.ds(pl.multiple_of(i * rb, rb), rb)
            val = jnp.dot(ctx[r, col], w_ref[...], preferred_element_type=jnp.float32)
            if first:
                acc[r, :] = val
            else:
                acc[r, :] += val
            return carry

        lax.fori_loop(0, n_blk, step, 0)

    for blk in range(n_blk // 2):
        c_from_left(blk).wait_recv()
        start(f_send(blk))
    add_shard(0, True)
    def pass_left(blk):
        c_from_right(blk).wait_recv()
        start(f_send(blk))

    def last_hop(i):
        for kind in range(2, 4):
            x_land(i, kind).wait_recv()
        start(t_send(i, 3))

    relay_x(2)
    for blk in range(n_blk // 2, n_blk - 1):
        pass_left(blk)
    last_hop(0)
    last_hop(1)
    pass_left(n_blk - 1)
    last_hop(2)

    def shard_in(i):
        for j in range(4):
            t_land(i, j).wait_recv()

    for blk in range(n_blk // 2, n_blk):
        c_from_left(blk).wait_recv()
    shard_in(0)
    add_shard(-1, False)
    for blk in range(n_blk // 2):
        c_from_right(blk).wait_recv()
    shard_in(1)
    add_shard(1, False)
    shard_in(2)

    col = pl.ds(pl.multiple_of(tp_of(2) * shard, 128), shard)
    h_copy = lambda blk: pltpu.make_async_copy(nv.at[pl.ds(blk * rb, rb), :], h_hbm.at[pl.ds(blk * rb, rb), :], hsem.at[blk])
    n_copy = lambda blk: pltpu.make_async_copy(ns.at[blk % 2], n_hbm.at[pl.ds(blk * rb, rb), :], nsem.at[blk])
    w_far = wo.at[tp_of(2)]
    for blk in range(n_blk):
        f_land(blk).wait_recv()
        x_again(blk).wait()
        if blk >= 2:
            n_copy(blk - 2).wait()
        r = pl.ds(blk * rb, rb)
        acc[r, :] += jnp.dot(ctx[r, col], w_far[...], preferred_element_type=jnp.float32)

        def end_step(i, carry, blk=blk):
            r = pl.ds(pl.multiple_of(blk * rb + i * nb, nb), nb)
            q = pl.ds(pl.multiple_of(i * nb, nb), nb)
            h = add_residual(xs[blk % 2, q, :], acc[r, :].astype(jnp.bfloat16))
            nv[r, :] = h
            ns[blk % 2, q, :] = rms_norm(h, g_ref[1:2, :])
            return carry

        lax.fori_loop(0, rb // nb, end_step, 0)
        h_copy(blk).start()
        n_copy(blk).start()
        if blk + 2 < n_blk:
            x_again(blk + 2).start()
    for blk in range(n_blk):
        h_copy(blk).wait()
        if blk >= n_blk - 2:
            n_copy(blk).wait()
    for copy in sent:
        copy.wait_send()


def front_call(x, s_len, gains, cos_full, sin_full, w_qkv, w_o, tp_size, side_size):
    rows, depth = x.shape
    n_kind, heads, _, head_dim = w_qkv.shape
    shard = heads * head_dim
    width = n_kind * shard
    rb = 256
    n_blk = rows // rb
    n_msg = 28 + 3 * n_blk
    act = jax.ShapeDtypeStruct((rows, depth), jnp.bfloat16)
    kv = jax.ShapeDtypeStruct((heads, rows, head_dim), jnp.bfloat16)
    dma = pltpu.SemaphoreType.DMA
    return pl.pallas_call(
        functools.partial(front_kernel, rb=rb, tp_size=tp_size, side_size=side_size),
        out_shape=(act, act, kv, kv),
        in_specs=[SM, VM, VM, VM, ANY, ANY, ANY],
        out_specs=(ANY, ANY, VM, VM),
        scratch_shapes=[
            pltpu.VMEM((2, rb, depth), jnp.bfloat16),
            pltpu.VMEM((2, rb, depth), jnp.bfloat16),
            pltpu.VMEM((rows, depth), jnp.bfloat16),
            pltpu.VMEM((depth, width), jnp.bfloat16),
            pltpu.VMEM((rows, depth), jnp.float32),
            pltpu.VMEM((heads, rows, head_dim), jnp.bfloat16),
            pltpu.VMEM((rows, tp_size * shard), jnp.bfloat16),
            pltpu.VMEM((tp_size, shard, depth), jnp.bfloat16),
            dma((n_kind * heads,)), dma((2 * n_blk,)), dma((1,)), dma((n_blk,)), dma((n_blk,)), dma((n_msg,)), dma((n_msg,)),
        ],
        compiler_params=pltpu.CompilerParams(vmem_limit_bytes=67043328, collective_id=0, has_side_effects=True),
        cost_estimate=pl.CostEstimate(flops=2 * rows * depth * (width + tp_size * shard), bytes_accessed=2 * (4 * rows * depth + depth * width), transcendentals=0),
        name="front",
    )(s_len, cos_full, sin_full, gains, x, w_qkv, w_o)


def back_kernel(h_hbm, n_hbm, wgu_hbm, wd_hbm, k_hbm, v_hbm, tok_ref, len_ref, cos_ref, sin_ref, dg_ref, wqd_hbm, wod_hbm, wgud_hbm, wdd_hbm, kc_hbm, vc_hbm, out_hbm, kp_hbm, vp_hbm, dec_ref, ktok_ref, vtok_ref, nv, act, gu_v, wd_v, part, land, hb, hres, relay, cbuf, dscr, dq, dprob, dctx, dpart, dland, dtok, dact, nsem, gsem, dsem, hsem, osem, qsem, dgsem, csem, ssem, rsem, *, fb, tp_size, side_size):
    ff, depth = wd_hbm.shape
    heads, rows, head_dim = k_hbm.shape
    chunk = rows // tp_size
    half = depth // 2
    sub = half // 2
    me = lax.axis_index('tp')
    side = lax.axis_index('side')
    tp_of = lambda d: lax.rem(me + d + tp_size, tp_size)
    to_right = {'tp': tp_of(1)}
    to_left = {'tp': tp_of(-1)}
    mate = lax.rem(side + side_size // 2, side_size)
    order = (-1, 1, 2, 0)
    pieces = [(f, min(fb, ff - f)) for f in range(0, ff, fb)]
    sent = []

    def start(copy):
        copy.start()
        sent.append(copy)

    def remote(idx, src, dst, dev):
        return pltpu.make_async_remote_copy(src_ref=src, dst_ref=dst, send_sem=ssem.at[idx], recv_sem=rsem.at[idx], device_id=dev, device_id_type=pl.DeviceIdType.MESH)

    def rows_of(d):
        return pl.ds(pl.multiple_of(tp_of(d) * chunk, chunk), chunk)

    def n_copy(c):
        return pltpu.make_async_copy(n_hbm.at[rows_of(order[c]), :], nv.at[pl.ds(c * chunk, chunk), :], nsem.at[c])

    def gu_copy(p, which):
        f, size = pieces[p]
        return pltpu.make_async_copy(wgu_hbm.at[which, pl.ds(f, size), :], gu_v.at[which, pl.ds(f, size), :], gsem.at[2 * p + which])

    wd_copy = pltpu.make_async_copy(wd_hbm, wd_v, dsem.at[0])
    h_copy = pltpu.make_async_copy(h_hbm.at[rows_of(0), :], hres, hsem.at[0])

    n_copy(0).start()
    n_copy(1).start()
    ahead = 3
    for p in range(ahead):
        gu_copy(p, 0).start()
        gu_copy(p, 1).start()

    barrier = pltpu.get_barrier_semaphore()
    peers = [{'tp': tp_of(d)} for d in range(1, tp_size)] + [{'tp': t, 'side': mate} for t in range(tp_size)]
    for dev in peers:
        pl.semaphore_signal(barrier, inc=1, device_id=dev, device_id_type=pl.DeviceIdType.MESH)
    pl.semaphore_wait(barrier, len(peers))

    def kv_send(i, src, dst, idx):
        head = me * heads + i
        return remote(idx, src.at[i], dst.at[head // tp_size], {'tp': lax.rem(head, tp_size), 'side': mate})

    def kv_land(i, src, dst, idx):
        slot = lax.rem(me - i + heads, heads)
        return remote(idx, src.at[i], dst.at[slot], {'tp': me, 'side': mate})

    far = tp_size // 2
    ways = ((1, k_hbm, kp_hbm), (-1, v_hbm, vp_hbm))

    def far_send(n):
        way, src, _ = ways[n]
        return remote(n * heads + far, src.at[far], relay.at[n], {'tp': tp_of(way), 'side': mate})

    def far_relay(n):
        way, _, dst = ways[n]
        head = tp_of(-way) * heads + far
        return remote(2 * heads + 36 + n, relay.at[n], dst.at[head // tp_size], {'tp': tp_of(way)})

    def far_land(n):
        way, _, dst = ways[n]
        return remote(2 * heads + 36 + n, relay.at[n], dst.at[lax.rem(me - far + heads, heads)], {'tp': tp_of(way)})

    for n in range(2):
        start(far_send(n))
    for i in range(heads):
        if i != far:
            start(kv_send(i, k_hbm, kp_hbm, i))
            start(kv_send(i, v_hbm, vp_hbm, heads + i))
    base = 2 * heads

    nt = (((1,), (1,)), ((), ()))
    span = 2 * chunk

    def gate_up(c, f, size):
        n_rows = nv[c * chunk:c * chunk + span, :]
        gate = lax.dot_general(n_rows, gu_v[0, f:f + size, :], nt, preferred_element_type=jnp.float32)
        up = lax.dot_general(n_rows, gu_v[1, f:f + size, :], nt, preferred_element_type=jnp.float32)
        gate = gate.astype(jnp.bfloat16).astype(jnp.float32)
        up = up.astype(jnp.bfloat16).astype(jnp.float32)
        act[:, f:f + size] = (gate * jax.nn.sigmoid(gate) * up).astype(jnp.bfloat16)

    def down(c, row, n_rows, lo):
        for col in range(lo, lo + half, fb):
            part[(c + row) * chunk:(c + row) * chunk + n_rows, col:col + fb] = jnp.dot(act[row * chunk:row * chunk + n_rows, :], wd_v[:, col:col + fb], preferred_element_type=jnp.float32)

    n_copy(0).wait()
    n_copy(1).wait()
    for p, (f, size) in enumerate(pieces):
        gu_copy(p, 0).wait()
        gu_copy(p, 1).wait()
        if p + ahead < len(pieces):
            gu_copy(p + ahead, 0).start()
            gu_copy(p + ahead, 1).start()
        if p + ahead == len(pieces):
            wd_copy.start()
            n_copy(2).start()
            n_copy(3).start()
            h_copy.start()
        gate_up(0, f, size)
    wd_copy.wait()

    cols = lambda way, q: pl.ds(way * half + q * sub, sub)
    devs = (to_right, to_left)

    def rs(step, way, q):
        idx = base + 4 * step + 2 * way + q
        dst = land.at[step, :, cols(way, q)]
        if step == 0:
            src = part.at[pl.ds(way * chunk, chunk), cols(way, q)]
        else:
            src = land.at[step - 1, :, cols(way, q)]
        return remote(idx, src, dst, devs[way])

    down(0, 0, chunk, 0)
    start(rs(0, 0, 0))
    start(rs(0, 0, 1))
    down(0, 1, chunk, half)
    start(rs(0, 1, 0))
    start(rs(0, 1, 1))
    down(0, 0, chunk, half)
    down(0, 1, chunk, 0)
    n_copy(2).wait()
    n_copy(3).wait()
    for f, size in pieces:
        gate_up(2, f, size)
    d_rows = tok_ref.shape[0]
    d_heads = heads
    shard = heads * head_dim
    n_kind = wqd_hbm.shape[0]
    cache_len = kc_hbm.shape[2]
    k_half = depth // 2
    lo_rows = 3 * head_dim

    def wq_copy(kind, head, hv):
        idx = kind * d_heads + head
        return pltpu.make_async_copy(wqd_hbm.at[kind, head, pl.ds(hv * k_half, k_half), :], gu_v.at[hv, pl.ds(0, k_half), pl.ds(idx * head_dim, head_dim)], qsem.at[2 * idx + hv])

    wo_lo = pltpu.make_async_copy(wod_hbm.at[pl.ds(0, lo_rows), :], gu_v.at[0, pl.ds(k_half, lo_rows), :], dsem.at[1])
    wo_hi = pltpu.make_async_copy(wod_hbm.at[pl.ds(lo_rows, shard - lo_rows), :], gu_v.at[1, pl.ds(k_half, shard - lo_rows), :], dsem.at[2])
    wdd_copy = pltpu.make_async_copy(wdd_hbm, wd_v, dsem.at[3])

    def gud_copy(p, which):
        f, size = pieces[p]
        return pltpu.make_async_copy(wgud_hbm.at[which, pl.ds(f, size), :], gu_v.at[which, pl.ds(f, size), :], dgsem.at[2 * p + which])

    def c_copy(src, b, slot):
        return pltpu.make_async_copy(src.at[b], cbuf.at[slot], csem.at[slot])

    for kind in range(n_kind):
        for head in range(d_heads):
            for hv in range(2):
                wq_copy(kind, head, hv).start()
    wo_lo.start()
    wo_hi.start()
    c_copy(kc_hbm, 0, 0).start()
    down(2, 0, span, 0)
    down(2, 0, span, half)
    wdd_copy.start()

    nb = 64
    slots = ((2, 2), (1, 0), (3, 3))

    def event(step, q):
        for way in range(2):
            rs(step, way, q).wait_recv()

            def add_step(i, carry, way=way):
                r = pl.ds(pl.multiple_of(i * nb, nb), nb)
                pr = pl.ds(pl.multiple_of(slots[step][way] * chunk + i * nb, nb), nb)
                land[step, r, cols(way, q)] += part[pr, cols(way, q)]
                return carry

            lax.fori_loop(0, chunk // nb, add_step, 0)
            start(rs(step + 1, way, q))

    def decode_qkv():
        normed = rms_norm(tok_ref[...], dg_ref[0:1, :])
        for kind in range(n_kind):
            for head in range(d_heads):
                for hv in range(2):
                    wq_copy(kind, head, hv).wait()
        cos_b = cos_ref[rows:rows + d_rows, :]
        sin_b = sin_ref[rows:rows + d_rows, :]
        for kind in range(n_kind):
            c0 = kind * shard
            val = jnp.dot(normed[:, :k_half], gu_v[0, 0:k_half, c0:c0 + shard], preferred_element_type=jnp.float32)
            val += jnp.dot(normed[:, k_half:], gu_v[1, 0:k_half, c0:c0 + shard], preferred_element_type=jnp.float32)
            for head in range(d_heads):
                one = val[:, head * head_dim:(head + 1) * head_dim]
                if kind < 2:
                    one = one * cos_b + pltpu.roll(one, head_dim // 2, 1) * sin_b
                (dq, ktok_ref, vtok_ref)[kind][head] = one.astype(jnp.bfloat16).astype(jnp.bfloat16 if kind == 0 else jnp.float32)

    row_id = lax.broadcasted_iota(jnp.int32, (d_rows, 1), 0)

    def over_rows(src, body):
        def step(b, carry):
            slot = lax.rem(b, 2)
            c_copy(src, b, slot).wait()

            @pl.when(b + 1 < d_rows)
            def _():
                c_copy(src, b + 1, 1 - slot).start()

            body(b, slot)
            return carry

        lax.fori_loop(0, d_rows, step, 0)

    def decode_scores():
        def body(b, slot):
            for head in range(d_heads):
                sc = lax.dot_general(dq[head], cbuf[slot, head], nt, preferred_element_type=jnp.float32)
                dscr[head] = jnp.where(row_id == b, sc, dscr[head])

        over_rows(kc_hbm, body)
        c_copy(vc_hbm, 0, 0).start()
        scale = head_dim ** -0.5
        pos = lax.broadcasted_iota(jnp.int32, (d_rows, cache_len), 1)
        seen = pos < len_ref[...]
        for head in range(d_heads):
            sc = jnp.where(seen, dscr[head] * scale, MASKED)
            own_sc = jnp.sum(dq[head].astype(jnp.float32) * ktok_ref[head].astype(jnp.float32), axis=-1, keepdims=True) * scale
            top = jnp.maximum(jnp.max(sc, axis=-1, keepdims=True), own_sc)
            ex = jnp.exp(sc - top)
            own_ex = jnp.exp(own_sc - top)
            den = jnp.sum(ex, axis=-1, keepdims=True) + own_ex
            dprob[head] = (ex / den).astype(jnp.bfloat16)
            own_p = (own_ex / den).astype(jnp.bfloat16).astype(jnp.float32)
            dctx[:, head * head_dim:(head + 1) * head_dim] = own_p * vtok_ref[head].astype(jnp.float32)

    def decode_context():
        def body(b, slot):
            for head in range(d_heads):
                got = jnp.dot(dprob[head], cbuf[slot, head], preferred_element_type=jnp.float32)
                hc = slice(head * head_dim, (head + 1) * head_dim)
                dctx[:, hc] += jnp.where(row_id == b, got, 0.0)

        over_rows(vc_hbm, body)
        wo_lo.wait()
        wo_hi.wait()
        ctx_b = dctx[...].astype(jnp.bfloat16)
        val = jnp.dot(ctx_b[:, :lo_rows], gu_v[0, k_half:k_half + lo_rows, :], preferred_element_type=jnp.float32)
        dpart[0] = val + jnp.dot(ctx_b[:, lo_rows:], gu_v[1, k_half:k_half + shard - lo_rows, :], preferred_element_type=jnp.float32)
        for p in range(len(pieces)):
            gud_copy(p, 0).start()
            gud_copy(p, 1).start()

    base_d = base + 24
    d_cols = lambda d: pl.ds(pl.multiple_of(tp_of(d) * shard, 128), shard)

    def d_scatter(n, d):
        return remote(base_d + 6 * n + d - 1, dpart.at[n, :, d_cols(d)], dland.at[n, d - 1], {'tp': tp_of(d)})

    def d_gather(n, d):
        return remote(base_d + 6 * n + 2 + d, dtok.at[n, :, d_cols(0)], dtok.at[n, :, d_cols(0)], {'tp': tp_of(d)})

    def d_gather_land(n, d):
        return remote(base_d + 6 * n + 2 + d, dtok.at[n, :, d_cols(-d)], dtok.at[n, :, d_cols(-d)], {'tp': tp_of(d)})

    def decode_scatter(n):
        for d in range(1, tp_size):
            start(d_scatter(n, d))

    def decode_sum(n, before):
        for d in range(1, tp_size):
            d_scatter(n, d).wait_recv()
        total = dpart[n, :, d_cols(0)]
        for d in range(1, tp_size):
            total = total + dland[n, d - 1]
        dtok[n, :, d_cols(0)] = add_residual(before[:, d_cols(0)], total.astype(jnp.bfloat16))
        for d in range(1, tp_size):
            start(d_gather(n, d))

    def decode_gathered(n):
        for d in range(1, tp_size):
            d_gather_land(n, d).wait_recv()

    def decode_gate_up(lo, hi):
        normed = rms_norm(dtok[0], dg_ref[1:2, :])
        for p in range(lo, hi):
            f, size = pieces[p]
            gud_copy(p, 0).wait()
            gud_copy(p, 1).wait()
            gate = lax.dot_general(normed, gu_v[0, f:f + size, :], nt, preferred_element_type=jnp.float32)
            up = lax.dot_general(normed, gu_v[1, f:f + size, :], nt, preferred_element_type=jnp.float32)
            gate = gate.astype(jnp.bfloat16).astype(jnp.float32)
            up = up.astype(jnp.bfloat16).astype(jnp.float32)
            dact[:, f:f + size] = (gate * jax.nn.sigmoid(gate) * up).astype(jnp.bfloat16)

    def decode_down():
        wdd_copy.wait()
        dpart[1] = jnp.dot(dact[...], wd_v[...], preferred_element_type=jnp.float32)

    event(0, 0)
    decode_qkv()
    event(0, 1)
    decode_scores()
    event(1, 0)
    for n in range(2):
        far_send(n).wait_recv()
        start(far_relay(n))
    decode_context()
    decode_scatter(0)
    event(1, 1)

    base_ag = base + 12
    h_copy.wait()

    def ag(way, q, dev_i):
        idx = base_ag + 4 * way + 2 * q + dev_i
        return remote(idx, hb.at[:, cols(way, q)], out_hbm.at[rows_of(0), cols(way, q)], devs[dev_i])

    def ag_land(way, q, dev_i):
        idx = base_ag + 4 * way + 2 * q + dev_i
        return remote(idx, hb.at[:, cols(way, q)], out_hbm.at[rows_of(-1 if dev_i == 0 else 1), cols(way, q)], devs[dev_i])

    def fwd(way, q):
        ref = out_hbm.at[rows_of(-1 if way == 0 else 1), cols(way, q)]
        return remote(base_ag + 8 + 2 * way + q, ref, ref, devs[way])

    def fwd_land(way, q):
        ref = out_hbm.at[rows_of(2), cols(way, q)]
        return remote(base_ag + 8 + 2 * way + q, ref, ref, devs[way])

    for q in range(2):
        for way in range(2):
            rs(2, way, q).wait_recv()

            def end_step(i, carry, way=way, q=q):
                r = pl.ds(pl.multiple_of(i * nb, nb), nb)
                pr = pl.ds(pl.multiple_of(3 * chunk + i * nb, nb), nb)
                total = land[2, r, cols(way, q)] + part[pr, cols(way, q)]
                hb[r, cols(way, q)] = add_residual(hres[r, cols(way, q)], total.astype(jnp.bfloat16))
                return carry

            lax.fori_loop(0, chunk // nb, end_step, 0)
            start(ag(way, q, way))
            start(ag(way, q, 1 - way))
        if q == 0:
            decode_sum(0, tok_ref)
    own = pltpu.make_async_copy(hb, out_hbm.at[rows_of(0), :], osem.at[0])
    own.start()
    decode_gathered(0)
    mid = len(pieces) // 2
    for q in range(2):
        for way in range(2):
            ag_land(way, q, way).wait_recv()
            start(fwd(way, q))
        decode_gate_up(q * mid, mid if q == 0 else len(pieces))
    decode_down()
    decode_scatter(1)
    decode_sum(1, dtok.at[0])
    for q in range(2):
        for way in range(2):
            ag_land(way, q, 1 - way).wait_recv()
    for i in range(heads):
        if i != far:
            kv_land(i, k_hbm, kp_hbm, i).wait_recv()
            kv_land(i, v_hbm, vp_hbm, heads + i).wait_recv()
    for n in range(2):
        far_land(n).wait_recv()
    for q in range(2):
        for way in range(2):
            fwd_land(way, q).wait_recv()
    own.wait()
    decode_gathered(1)
    dec_ref[...] = dtok[1]
    for copy in sent:
        copy.wait_send()


def back_call(h, normed, w_gu, w_down, k, v, dec, tp_size, side_size):
    rows, depth = h.shape
    ff = w_down.shape[0]
    heads = k.shape[0]
    chunk = rows // tp_size
    fb = 256
    n_piece = -(-ff // fb)
    n_msg = 2 * heads + 12 + 12 + 12 + 2
    d_rows = dec[0].shape[0]
    head_dim = k.shape[2]
    cache_len = dec[9].shape[2]
    dma = pltpu.SemaphoreType.DMA
    bf16 = jnp.bfloat16
    kv = jax.ShapeDtypeStruct(k.shape, bf16)
    return pl.pallas_call(
        functools.partial(back_kernel, fb=fb, tp_size=tp_size, side_size=side_size),
        out_shape=(jax.ShapeDtypeStruct((rows, depth), bf16), kv, kv, jax.ShapeDtypeStruct((d_rows, depth), bf16)) + (jax.ShapeDtypeStruct((heads, d_rows, head_dim), jnp.float32),) * 2,
        in_specs=[ANY] * 6 + [VM] * 5 + [ANY] * 6,
        out_specs=(ANY,) * 3 + (VM,) * 3,
        scratch_shapes=[
            pltpu.VMEM((rows, depth), bf16),
            pltpu.VMEM((2 * chunk, ff), bf16),
            pltpu.VMEM((2, ff, depth), bf16),
            pltpu.VMEM((ff, depth), bf16),
            pltpu.VMEM((rows, depth), jnp.float32),
            pltpu.VMEM((3, chunk, depth), jnp.float32),
            pltpu.VMEM((chunk, depth), bf16),
            pltpu.VMEM((chunk, depth), bf16),
            pltpu.VMEM((2, rows, head_dim), bf16),
            pltpu.VMEM((2, heads, cache_len, head_dim), bf16),
            pltpu.VMEM((heads, d_rows, cache_len), jnp.float32),
            pltpu.VMEM((heads, d_rows, head_dim), bf16),
            pltpu.VMEM((heads, d_rows, cache_len), bf16),
            pltpu.VMEM((d_rows, heads * head_dim), jnp.float32),
            pltpu.VMEM((2, d_rows, depth), jnp.float32),
            pltpu.VMEM((2, tp_size - 1, d_rows, heads * head_dim), jnp.float32),
            pltpu.VMEM((2, d_rows, depth), bf16),
            pltpu.VMEM((d_rows, ff), bf16),
            dma((tp_size,)), dma((2 * n_piece,)), dma((4,)), dma((1,)), dma((1,)), dma((6 * heads,)), dma((2 * n_piece,)), dma((2,)), dma((n_msg,)), dma((n_msg,)),
        ],
        compiler_params=pltpu.CompilerParams(vmem_limit_bytes=67043328, collective_id=1, has_side_effects=True),
        cost_estimate=pl.CostEstimate(flops=6 * rows * ff * depth, bytes_accessed=6 * ff * depth + 8 * rows * depth, transcendentals=0),
        name="back",
    )(h, normed, w_gu, w_down, k, v, *dec)


def cache_kernel(len_ref, kt_ref, vt_ref, k_ref, v_ref, ko_ref, vo_ref):
    n_rows, heads, cache_len, head_dim = k_ref.shape
    first = pl.program_id(0) * n_rows
    pos = lax.broadcasted_iota(jnp.int32, (cache_len, head_dim), 0)
    for j in range(n_rows):
        here = pos == len_ref[first + j]
        for head in range(heads):
            for tok, src, dst in ((kt_ref, k_ref, ko_ref), (vt_ref, v_ref, vo_ref)):
                new = tok[head, pl.ds(first + j, 1), :]
                dst[j, head] = jnp.where(here, new, src[j, head].astype(jnp.float32)).astype(dst.dtype)


def cache_call(c_len, k_tok, v_tok, k_cache, v_cache):
    d_rows, heads, cache_len, head_dim = k_cache.shape
    step = 2
    block = pl.BlockSpec((step, heads, cache_len, head_dim), lambda i: (i, 0, 0, 0))
    out = jax.ShapeDtypeStruct(k_cache.shape, k_cache.dtype)
    return pl.pallas_call(
        cache_kernel,
        grid=(d_rows // step,),
        out_shape=(out, out),
        in_specs=[SM, VM, VM, block, block],
        out_specs=(block, block),
        compiler_params=pltpu.CompilerParams(vmem_limit_bytes=67043328),
        cost_estimate=pl.CostEstimate(flops=k_cache.size, bytes_accessed=8 * k_cache.size, transcendentals=0),
        name="cache",
    )(c_len, k_tok, v_tok, k_cache, v_cache)


def run_layers(prompt, s_len, pre, tokens, k_cache, v_cache, c_len, dec, tp_size, side_size):
    w_qkv, w_out, w_gu, w_down, gains = pre
    dw_qkv, dw_out, dw_gu, dw_down, dgains = dec
    rows, width = prompt.shape
    layers, _, _, heads_loc, head_dim = w_qkv.shape
    shard = heads_loc * head_dim
    d_rows, cache_len = k_cache.shape[1:3]

    cos_tab, sin_tab = rope_tables(jnp.concatenate([jnp.arange(rows, dtype=jnp.int32), c_len]), head_dim)
    cos_full = jnp.concatenate([cos_tab, cos_tab], axis=-1)
    sin_full = jnp.concatenate([-sin_tab, sin_tab], axis=-1)
    hidden = prompt
    outs = []
    for layer in range(layers):
        w_t = w_qkv[layer].transpose(1, 2, 0, 3)
        hidden, normed, k, v = front_call(hidden, s_len, gains[layer], cos_full, sin_full, w_t, w_out[layer].reshape(shard, width), tp_size, side_size)
        by_head = lambda cache: cache[layer].reshape(d_rows, cache_len, heads_loc, head_dim).transpose(0, 2, 1, 3)
        dec_args = (tokens, c_len[:, None], cos_full, sin_full, dgains[layer], dw_qkv[layer].reshape(width, 3, heads_loc, head_dim).transpose(1, 2, 0, 3), dw_out[layer].reshape(shard, width), dw_gu[layer], dw_down[layer], by_head(k_cache), by_head(v_cache))
        hidden, k_inst, v_inst, tokens, k_tok, v_tok = back_call(hidden, normed, w_gu[layer], w_down[layer], k, v, dec_args, tp_size, side_size)
        k_new, v_new = cache_call(c_len, k_tok, v_tok, by_head(k_cache), by_head(v_cache))
        as_cache = lambda new: new.transpose(0, 2, 1, 3)[:, :, :, None, :]
        outs.append((k_inst.transpose(1, 0, 2)[:, :, None, :], v_inst.transpose(1, 0, 2)[:, :, None, :], as_cache(k_new), as_cache(v_new)))
    return (hidden, tokens) + tuple(jnp.stack(parts) for parts in zip(*outs))


def solution(mesh):
    tp_size = mesh.shape['tp']
    side_size = mesh.shape['side']
    inst_axes = ('pair', 'side')
    rows_spec = P(inst_axes, None)
    vec_spec = P(inst_axes)
    cache_spec = P(None, inst_axes, None, None, 'tp', None)
    prompt_spec = P(None, inst_axes, None, 'tp', None)
    in_specs = (rows_spec, vec_spec, P(None, None, None, 'tp', None), P(None, 'tp', None, None), P(None, None, 'tp', None), P(None, 'tp', None), P(None, None, None), rows_spec, cache_spec, cache_spec, vec_spec, P(None, None, None, None, 'tp', None), P(None, None, 'tp', None, None), P(None, None, 'tp', None), P(None, 'tp', None), P(None, None, None))
    out_specs = (rows_spec, rows_spec, prompt_spec, prompt_spec, cache_spec, cache_spec)

    def device_fn(prompt_x, s_len, w_qkv_pre, w_out_pre, w_gu_pre, w_down_pre, gain_pre, dec_tokens, k_cache, v_cache, c_len, w_qkv_dec, w_out_dec, w_gu_dec, w_down_dec, gain_dec):
        pre = (w_qkv_pre, w_out_pre, w_gu_pre, w_down_pre, gain_pre)
        dec = (w_qkv_dec, w_out_dec, w_gu_dec, w_down_dec, gain_dec)
        return run_layers(prompt_x, s_len, pre, dec_tokens, k_cache, v_cache, c_len, dec, tp_size, side_size)

    return jax.shard_map(device_fn, mesh=mesh, in_specs=in_specs, out_specs=out_specs, check_vma=False)
```

```python
import functools

import jax
import jax.numpy as jnp
from jax import lax
from jax.experimental import pallas as pl
from jax.experimental.pallas import tpu as pltpu
from jax.sharding import PartitionSpec as P

EPSILON = 1e-6
THETA = 10000.0
MASKED = -1e30
VMEM_LIMIT = 60 * 1024 * 1024
ANY = pl.BlockSpec(memory_space=pl.ANY)
VM = pl.BlockSpec(memory_space=pltpu.VMEM)
SM = pl.BlockSpec(memory_space=pltpu.SMEM)


def rms_norm(hidden, gain_vec):
    hid_f32 = hidden.astype(jnp.float32)
    inv_rms = lax.rsqrt(jnp.mean(hid_f32 * hid_f32, axis=-1, keepdims=True) + EPSILON)
    return (hid_f32 * inv_rms * gain_vec).astype(jnp.bfloat16)


def add_residual(hidden, update):
    return (hidden.astype(jnp.float32) + update.astype(jnp.float32)).astype(jnp.bfloat16)


def rope_tables(positions, head_dim):
    half_dim = head_dim // 2
    inv_freq = THETA ** (-jnp.arange(half_dim, dtype=jnp.float32) * 2.0 / head_dim)
    angles = positions.astype(jnp.float32)[:, None] * inv_freq[None, :]
    return jnp.cos(angles), jnp.sin(angles)


def front_kernel(len_ref, cos_ref, sin_ref, g_ref, x_hbm, wqkv_hbm, wo_hbm, h_hbm, n_hbm, k_ref, v_ref, xs, ns, nv, wv, acc, qv, ctx, wo, wsem, xsem, osem, hsem, nsem, ssem, rsem, *, rb, tp_size, side_size):
    n_kind, heads, depth, head_dim = wqkv_hbm.shape
    rows = x_hbm.shape[0]
    n_blk = rows // rb
    shard = heads * head_dim
    width = n_kind * shard
    half = depth // 2
    me = lax.axis_index('tp')
    side = lax.axis_index('side')
    core = lax.rem(side, 2)
    chip = side // 2
    n_chip = side_size // 2
    part = shard // side_size
    tp_of = lambda d: lax.rem(me + d + tp_size, tp_size)
    chip_of = lambda d: lax.rem(chip + d + n_chip, n_chip)
    to_right = {'tp': tp_of(1)}
    to_left = {'tp': tp_of(-1)}
    to_up = {'side': chip_of(1) * 2 + core}
    to_down = {'side': chip_of(-1) * 2 + core}
    to_twin = {'side': chip * 2 + 1 - core}
    whole = pl.ds(0, depth)
    cols_a = pl.ds(0, half)
    cols_b = pl.ds(half, half)

    def send(idx, ref, dev, src=None):
        return pltpu.make_async_remote_copy(src_ref=ref if src is None else src, dst_ref=ref, send_sem=ssem.at[idx], recv_sem=rsem.at[idx], device_id=dev, device_id_type=pl.DeviceIdType.MESH)

    def w_part(d_tp, d_chip, cols, core_id):
        row0 = pl.multiple_of((chip_of(d_chip) * 2 + core_id) * part, 16)
        return wo.at[tp_of(d_tp), pl.ds(row0, part), cols]

    def c_part(d_tp, blk):
        return ctx.at[pl.ds(blk * rb, rb), pl.ds(pl.multiple_of(tp_of(d_tp) * shard, 128), shard)]

    offs = (-1, 1, 2)
    hops = (0, -1, 1, 2)
    sent = []

    def start(copy):
        copy.start()
        sent.append(copy)

    own_slice = wo_hbm.at[pl.ds(pl.multiple_of(side * part, 16), part), :]
    y_send = [
        lambda: send(0, w_part(0, 0, whole, core), to_right, src=own_slice),
        lambda: send(1, w_part(0, 0, whole, core), to_left, src=own_slice),
        lambda: send(2, w_part(-1, 0, cols_a, core), to_right),
        lambda: send(3, w_part(1, 0, cols_b, core), to_left),
    ]
    y_land = [
        lambda: send(0, w_part(-1, 0, whole, core), to_right),
        lambda: send(1, w_part(1, 0, whole, core), to_left),
        lambda: send(2, w_part(-2, 0, cols_a, core), to_right),
        lambda: send(3, w_part(2, 0, cols_b, core), to_left),
    ]

    def x_send(i, kind):
        d = offs[i]
        idx = 4 + 4 * i + kind
        if kind == 0:
            return send(idx, w_part(d, 0, whole, core), to_up)
        if kind == 1:
            return send(idx, w_part(d, 0, whole, core), to_down)
        if kind == 2:
            return send(idx, w_part(d, -1, cols_a, core), to_up)
        return send(idx, w_part(d, 1, cols_b, core), to_down)

    def x_land(i, kind):
        d = offs[i]
        idx = 4 + 4 * i + kind
        if kind == 0:
            return send(idx, w_part(d, -1, whole, core), to_up)
        if kind == 1:
            return send(idx, w_part(d, 1, whole, core), to_down)
        if kind == 2:
            return send(idx, w_part(d, -2, cols_a, core), to_up)
        return send(idx, w_part(d, 2, cols_b, core), to_down)

    def t_send(i, j):
        return send(16 + 4 * i + j, w_part(offs[i], hops[j], whole, core), to_twin)

    def t_land(i, j):
        return send(16 + 4 * i + j, w_part(offs[i], hops[j], whole, 1 - core), to_twin)

    c_right = lambda blk: send(28 + blk, c_part(0, blk), to_right)
    c_left = lambda blk: send(28 + n_blk + blk, c_part(0, blk), to_left)
    c_from_left = lambda blk: send(28 + blk, c_part(-1, blk), to_right)
    c_from_right = lambda blk: send(28 + n_blk + blk, c_part(1, blk), to_left)

    def f_send(blk):
        if blk < n_blk // 2:
            return send(28 + 2 * n_blk + blk, c_part(-1, blk), to_right)
        return send(28 + 2 * n_blk + blk, c_part(1, blk), to_left)

    def f_land(blk):
        return send(28 + 2 * n_blk + blk, c_part(2, blk), to_right if blk < n_blk // 2 else to_left)

    def w_copy(kind, head):
        idx = kind * heads + head
        return pltpu.make_async_copy(wqkv_hbm.at[kind, head], wv.at[:, pl.ds(idx * head_dim, head_dim)], wsem.at[idx])

    x_in = lambda blk: pltpu.make_async_copy(x_hbm.at[pl.ds(blk * rb, rb), :], nv.at[pl.ds(blk * rb, rb), :], xsem.at[blk])
    x_again = lambda blk: pltpu.make_async_copy(x_hbm.at[pl.ds(blk * rb, rb), :], xs.at[blk % 2], xsem.at[n_blk + blk])
    own_w = pltpu.make_async_copy(wo_hbm, wo.at[me], osem.at[0])

    for blk in range(n_blk):
        x_in(blk).start()
    for kind in range(n_kind):
        for head in range(heads):
            w_copy(kind, head).start()
    own_w.start()
    x_again(0).start()
    x_again(1).start()

    barrier = pltpu.get_barrier_semaphore()
    for dev in (to_right, to_left, to_up, to_down, to_twin):
        pl.semaphore_signal(barrier, inc=1, device_id=dev, device_id_type=pl.DeviceIdType.MESH)
    pl.semaphore_wait(barrier, 5)
    start(y_send[0]())
    start(y_send[1]())

    nb = 64
    for blk in range(n_blk):
        x_in(blk).wait()

    def norm_step(i, carry):
        r = pl.ds(pl.multiple_of(i * nb, nb), nb)
        nv[r, :] = rms_norm(nv[r, :], g_ref[0:1, :])
        return carry

    lax.fori_loop(0, rows // nb, norm_step, 0)
    for kind in range(n_kind):
        for head in range(heads):
            w_copy(kind, head).wait()

    def qkv_step(i, carry):
        r = pl.ds(pl.multiple_of(i * rb, rb), rb)
        acc[pl.ds(0, rb), pl.ds(0, width)] = jnp.dot(nv[r, :], wv[...], preferred_element_type=jnp.float32)
        cos_b = cos_ref[r, :]
        sin_b = sin_ref[r, :]
        for head in range(heads):
            for kind, out in ((0, qv), (1, k_ref)):
                idx = (kind * heads + head) * head_dim
                val = acc[0:rb, idx:idx + head_dim]
                out[head, r, :] = (val * cos_b + pltpu.roll(val, head_dim // 2, 1) * sin_b).astype(jnp.bfloat16)
            idx = (2 * heads + head) * head_dim
            v_ref[head, r, :] = acc[0:rb, idx:idx + head_dim].astype(jnp.bfloat16)
        return carry

    lax.fori_loop(0, n_blk // 2, qkv_step, 0)
    for m in range(2):
        y_land[m]().wait_recv()
    for m in range(2):
        start(y_send[2 + m]())
    for i in range(2):
        start(x_send(i, 0))
        start(x_send(i, 1))
        start(t_send(i, 0))
    lax.fori_loop(n_blk // 2, n_blk, qkv_step, 0)
    for m in range(2):
        y_land[2 + m]().wait_recv()
    start(x_send(2, 0))
    start(x_send(2, 1))
    start(t_send(2, 0))

    valid = len_ref[0]
    scale = head_dim ** -0.5
    for blk in range(n_blk):
        span = (blk + 1) * rb
        rowi = lax.broadcasted_iota(jnp.int32, (rb, span), 0) + blk * rb
        coli = lax.broadcasted_iota(jnp.int32, (rb, span), 1)
        seen = (coli <= rowi) & (coli < valid)

        def head_step(head, carry, blk=blk, span=span, seen=seen):
            kk = k_ref[head, pl.ds(0, span), :]
            s = lax.dot_general(qv[head, pl.ds(blk * rb, rb), :], kk, (((1,), (1,)), ((), ())), preferred_element_type=jnp.float32)
            s = jnp.where(seen, s * scale, MASKED)
            p = jnp.exp(s - jnp.max(s, axis=-1, keepdims=True))
            p = (p * (1.0 / jnp.sum(p, axis=-1, keepdims=True))).astype(jnp.bfloat16)
            c = jnp.dot(p, v_ref[head, pl.ds(0, span), :], preferred_element_type=jnp.float32).astype(jnp.bfloat16)
            ctx[pl.ds(blk * rb, rb), pl.ds(pl.multiple_of(me * shard + head * head_dim, head_dim), head_dim)] = c
            return carry

        lax.fori_loop(0, heads, head_step, 0)
        start(c_right(blk))
        start(c_left(blk))

    def relay_x(i):
        for kind in range(2):
            x_land(i, kind).wait_recv()
        for kind in range(2):
            start(x_send(i, 2 + kind))
        start(t_send(i, 1))
        start(t_send(i, 2))

    relay_x(0)
    relay_x(1)
    own_w.wait()

    def add_shard(d, first):
        w_ref = wo.at[tp_of(d)]
        col = pl.ds(pl.multiple_of(tp_of(d) * shard, 128), shard)

        def step(i, carry):
            r = pl.ds(pl.multiple_of(i * rb, rb), rb)
            val = jnp.dot(ctx[r, col], w_ref[...], preferred_element_type=jnp.float32)
            if first:
                acc[r, :] = val
            else:
                acc[r, :] += val
            return carry

        lax.fori_loop(0, n_blk, step, 0)

    for blk in range(n_blk // 2):
        c_from_left(blk).wait_recv()
        start(f_send(blk))
    add_shard(0, True)
    def pass_left(blk):
        c_from_right(blk).wait_recv()
        start(f_send(blk))

    def last_hop(i):
        for kind in range(2, 4):
            x_land(i, kind).wait_recv()
        start(t_send(i, 3))

    relay_x(2)
    for blk in range(n_blk // 2, n_blk - 1):
        pass_left(blk)
    last_hop(0)
    last_hop(1)
    pass_left(n_blk - 1)
    last_hop(2)

    def shard_in(i):
        for j in range(4):
            t_land(i, j).wait_recv()

    for blk in range(n_blk // 2, n_blk):
        c_from_left(blk).wait_recv()
    shard_in(0)
    add_shard(-1, False)
    for blk in range(n_blk // 2):
        c_from_right(blk).wait_recv()
    shard_in(1)
    add_shard(1, False)
    shard_in(2)

    col = pl.ds(pl.multiple_of(tp_of(2) * shard, 128), shard)
    h_copy = lambda blk: pltpu.make_async_copy(nv.at[pl.ds(blk * rb, rb), :], h_hbm.at[pl.ds(blk * rb, rb), :], hsem.at[blk])
    n_copy = lambda blk: pltpu.make_async_copy(ns.at[blk % 2], n_hbm.at[pl.ds(blk * rb, rb), :], nsem.at[blk])
    w_far = wo.at[tp_of(2)]
    for blk in range(n_blk):
        f_land(blk).wait_recv()
        x_again(blk).wait()
        if blk >= 2:
            n_copy(blk - 2).wait()
        r = pl.ds(blk * rb, rb)
        acc[r, :] += jnp.dot(ctx[r, col], w_far[...], preferred_element_type=jnp.float32)

        def end_step(i, carry, blk=blk):
            r = pl.ds(pl.multiple_of(blk * rb + i * nb, nb), nb)
            q = pl.ds(pl.multiple_of(i * nb, nb), nb)
            h = add_residual(xs[blk % 2, q, :], acc[r, :].astype(jnp.bfloat16))
            nv[r, :] = h
            ns[blk % 2, q, :] = rms_norm(h, g_ref[1:2, :])
            return carry

        lax.fori_loop(0, rb // nb, end_step, 0)
        h_copy(blk).start()
        n_copy(blk).start()
        if blk + 2 < n_blk:
            x_again(blk + 2).start()
    for blk in range(n_blk):
        h_copy(blk).wait()
        if blk >= n_blk - 2:
            n_copy(blk).wait()
    for copy in sent:
        copy.wait_send()


def front_call(x, s_len, gains, cos_full, sin_full, w_qkv, w_o, tp_size, side_size):
    rows, depth = x.shape
    n_kind, heads, _, head_dim = w_qkv.shape
    shard = heads * head_dim
    width = n_kind * shard
    rb = 256
    n_blk = rows // rb
    n_msg = 28 + 3 * n_blk
    act = jax.ShapeDtypeStruct((rows, depth), jnp.bfloat16)
    kv = jax.ShapeDtypeStruct((heads, rows, head_dim), jnp.bfloat16)
    dma = pltpu.SemaphoreType.DMA
    return pl.pallas_call(
        functools.partial(front_kernel, rb=rb, tp_size=tp_size, side_size=side_size),
        out_shape=(act, act, kv, kv),
        in_specs=[SM, VM, VM, VM, ANY, ANY, ANY],
        out_specs=(ANY, ANY, VM, VM),
        scratch_shapes=[
            pltpu.VMEM((2, rb, depth), jnp.bfloat16),
            pltpu.VMEM((2, rb, depth), jnp.bfloat16),
            pltpu.VMEM((rows, depth), jnp.bfloat16),
            pltpu.VMEM((depth, width), jnp.bfloat16),
            pltpu.VMEM((rows, depth), jnp.float32),
            pltpu.VMEM((heads, rows, head_dim), jnp.bfloat16),
            pltpu.VMEM((rows, tp_size * shard), jnp.bfloat16),
            pltpu.VMEM((tp_size, shard, depth), jnp.bfloat16),
            dma((n_kind * heads,)), dma((2 * n_blk,)), dma((1,)), dma((n_blk,)), dma((n_blk,)), dma((n_msg,)), dma((n_msg,)),
        ],
        compiler_params=pltpu.CompilerParams(vmem_limit_bytes=67043328, collective_id=0, has_side_effects=True),
        cost_estimate=pl.CostEstimate(flops=2 * rows * depth * (width + tp_size * shard), bytes_accessed=2 * (4 * rows * depth + depth * width), transcendentals=0),
        name="front",
    )(s_len, cos_full, sin_full, gains, x, w_qkv, w_o)


def back_kernel(h_hbm, n_hbm, wgu_hbm, wd_hbm, k_hbm, v_hbm, tok_ref, len_ref, cos_ref, sin_ref, dg_ref, wqd_hbm, wod_hbm, wgud_hbm, wdd_hbm, kc_hbm, vc_hbm, out_hbm, kp_hbm, vp_hbm, dec_ref, ktok_ref, vtok_ref, nv, act, gu_v, wd_v, part, land, hb, hres, relay, cbuf, dscr, dq, dprob, dctx, dpart, dland, dtok, dact, nsem, gsem, dsem, hsem, osem, qsem, dgsem, csem, ssem, rsem, *, fb, tp_size, side_size):
    ff, depth = wd_hbm.shape
    heads, rows, head_dim = k_hbm.shape
    chunk = rows // tp_size
    half = depth // 2
    sub = half // 2
    me = lax.axis_index('tp')
    side = lax.axis_index('side')
    tp_of = lambda d: lax.rem(me + d + tp_size, tp_size)
    to_right = {'tp': tp_of(1)}
    to_left = {'tp': tp_of(-1)}
    mate = lax.rem(side + side_size // 2, side_size)
    order = (-1, 1, 2, 0)
    pieces = [(f, min(fb, ff - f)) for f in range(0, ff, fb)]
    sent = []

    def start(copy):
        copy.start()
        sent.append(copy)

    def remote(idx, src, dst, dev):
        return pltpu.make_async_remote_copy(src_ref=src, dst_ref=dst, send_sem=ssem.at[idx], recv_sem=rsem.at[idx], device_id=dev, device_id_type=pl.DeviceIdType.MESH)

    def rows_of(d):
        return pl.ds(pl.multiple_of(tp_of(d) * chunk, chunk), chunk)

    def n_copy(c):
        return pltpu.make_async_copy(n_hbm.at[rows_of(order[c]), :], nv.at[pl.ds(c * chunk, chunk), :], nsem.at[c])

    def gu_copy(p, which):
        f, size = pieces[p]
        return pltpu.make_async_copy(wgu_hbm.at[which, pl.ds(f, size), :], gu_v.at[which, pl.ds(f, size), :], gsem.at[2 * p + which])

    wd_copy = pltpu.make_async_copy(wd_hbm, wd_v, dsem.at[0])
    h_copy = pltpu.make_async_copy(h_hbm.at[rows_of(0), :], hres, hsem.at[0])

    n_copy(0).start()
    n_copy(1).start()
    ahead = 3
    for p in range(ahead):
        gu_copy(p, 0).start()
        gu_copy(p, 1).start()

    barrier = pltpu.get_barrier_semaphore()
    peers = [{'tp': tp_of(d)} for d in range(1, tp_size)] + [{'tp': t, 'side': mate} for t in range(tp_size)]
    for dev in peers:
        pl.semaphore_signal(barrier, inc=1, device_id=dev, device_id_type=pl.DeviceIdType.MESH)
    pl.semaphore_wait(barrier, len(peers))

    def kv_send(i, src, dst, idx):
        head = me * heads + i
        return remote(idx, src.at[i], dst.at[head // tp_size], {'tp': lax.rem(head, tp_size), 'side': mate})

    def kv_land(i, src, dst, idx):
        slot = lax.rem(me - i + heads, heads)
        return remote(idx, src.at[i], dst.at[slot], {'tp': me, 'side': mate})

    far = tp_size // 2
    ways = ((1, k_hbm, kp_hbm), (-1, v_hbm, vp_hbm))

    def far_send(n):
        way, src, _ = ways[n]
        return remote(n * heads + far, src.at[far], relay.at[n], {'tp': tp_of(way), 'side': mate})

    def far_relay(n):
        way, _, dst = ways[n]
        head = tp_of(-way) * heads + far
        return remote(2 * heads + 36 + n, relay.at[n], dst.at[head // tp_size], {'tp': tp_of(way)})

    def far_land(n):
        way, _, dst = ways[n]
        return remote(2 * heads + 36 + n, relay.at[n], dst.at[lax.rem(me - far + heads, heads)], {'tp': tp_of(way)})

    for n in range(2):
        start(far_send(n))
    for i in range(heads):
        if i != far:
            start(kv_send(i, k_hbm, kp_hbm, i))
            start(kv_send(i, v_hbm, vp_hbm, heads + i))
    base = 2 * heads

    nt = (((1,), (1,)), ((), ()))
    span = 2 * chunk

    def gate_up(c, f, size):
        n_rows = nv[c * chunk:c * chunk + span, :]
        gate = lax.dot_general(n_rows, gu_v[0, f:f + size, :], nt, preferred_element_type=jnp.float32)
        up = lax.dot_general(n_rows, gu_v[1, f:f + size, :], nt, preferred_element_type=jnp.float32)
        gate = gate.astype(jnp.bfloat16).astype(jnp.float32)
        up = up.astype(jnp.bfloat16).astype(jnp.float32)
        act[:, f:f + size] = (gate * jax.nn.sigmoid(gate) * up).astype(jnp.bfloat16)

    def down(c, row, n_rows, lo):
        for col in range(lo, lo + half, fb):
            part[(c + row) * chunk:(c + row) * chunk + n_rows, col:col + fb] = jnp.dot(act[row * chunk:row * chunk + n_rows, :], wd_v[:, col:col + fb], preferred_element_type=jnp.float32)

    n_copy(0).wait()
    n_copy(1).wait()
    for p, (f, size) in enumerate(pieces):
        gu_copy(p, 0).wait()
        gu_copy(p, 1).wait()
        if p + ahead < len(pieces):
            gu_copy(p + ahead, 0).start()
            gu_copy(p + ahead, 1).start()
        if p + ahead == len(pieces):
            wd_copy.start()
            n_copy(2).start()
            n_copy(3).start()
            h_copy.start()
        gate_up(0, f, size)
    wd_copy.wait()

    cols = lambda way, q: pl.ds(way * half + q * sub, sub)
    devs = (to_right, to_left)

    def rs(step, way, q):
        idx = base + 4 * step + 2 * way + q
        dst = land.at[step, :, cols(way, q)]
        if step == 0:
            src = part.at[pl.ds(way * chunk, chunk), cols(way, q)]
        else:
            src = land.at[step - 1, :, cols(way, q)]
        return remote(idx, src, dst, devs[way])

    down(0, 0, chunk, 0)
    start(rs(0, 0, 0))
    start(rs(0, 0, 1))
    down(0, 1, chunk, half)
    start(rs(0, 1, 0))
    start(rs(0, 1, 1))
    down(0, 0, chunk, half)
    down(0, 1, chunk, 0)
    n_copy(2).wait()
    n_copy(3).wait()
    for f, size in pieces:
        gate_up(2, f, size)
    d_rows = tok_ref.shape[0]
    d_heads = heads
    shard = heads * head_dim
    n_kind = wqd_hbm.shape[0]
    cache_len = kc_hbm.shape[2]
    k_half = depth // 2
    lo_rows = 3 * head_dim

    def wq_copy(kind, head, hv):
        idx = kind * d_heads + head
        return pltpu.make_async_copy(wqd_hbm.at[kind, head, pl.ds(hv * k_half, k_half), :], gu_v.at[hv, pl.ds(0, k_half), pl.ds(idx * head_dim, head_dim)], qsem.at[2 * idx + hv])

    wo_lo = pltpu.make_async_copy(wod_hbm.at[pl.ds(0, lo_rows), :], gu_v.at[0, pl.ds(k_half, lo_rows), :], dsem.at[1])
    wo_hi = pltpu.make_async_copy(wod_hbm.at[pl.ds(lo_rows, shard - lo_rows), :], gu_v.at[1, pl.ds(k_half, shard - lo_rows), :], dsem.at[2])
    wdd_copy = pltpu.make_async_copy(wdd_hbm, wd_v, dsem.at[3])

    def gud_copy(p, which):
        f, size = pieces[p]
        return pltpu.make_async_copy(wgud_hbm.at[which, pl.ds(f, size), :], gu_v.at[which, pl.ds(f, size), :], dgsem.at[2 * p + which])

    def c_copy(src, b, slot):
        return pltpu.make_async_copy(src.at[b], cbuf.at[slot], csem.at[slot])

    for kind in range(n_kind):
        for head in range(d_heads):
            for hv in range(2):
                wq_copy(kind, head, hv).start()
    wo_lo.start()
    wo_hi.start()
    c_copy(kc_hbm, 0, 0).start()
    down(2, 0, span, 0)
    down(2, 0, span, half)
    wdd_copy.start()

    nb = 64
    slots = ((2, 2), (1, 0), (3, 3))

    def event(step, q):
        for way in range(2):
            rs(step, way, q).wait_recv()

            def add_step(i, carry, way=way):
                r = pl.ds(pl.multiple_of(i * nb, nb), nb)
                pr = pl.ds(pl.multiple_of(slots[step][way] * chunk + i * nb, nb), nb)
                land[step, r, cols(way, q)] += part[pr, cols(way, q)]
                return carry

            lax.fori_loop(0, chunk // nb, add_step, 0)
            start(rs(step + 1, way, q))

    def decode_qkv():
        normed = rms_norm(tok_ref[...], dg_ref[0:1, :])
        for kind in range(n_kind):
            for head in range(d_heads):
                for hv in range(2):
                    wq_copy(kind, head, hv).wait()
        cos_b = cos_ref[rows:rows + d_rows, :]
        sin_b = sin_ref[rows:rows + d_rows, :]
        for kind in range(n_kind):
            c0 = kind * shard
            val = jnp.dot(normed[:, :k_half], gu_v[0, 0:k_half, c0:c0 + shard], preferred_element_type=jnp.float32)
            val += jnp.dot(normed[:, k_half:], gu_v[1, 0:k_half, c0:c0 + shard], preferred_element_type=jnp.float32)
            for head in range(d_heads):
                one = val[:, head * head_dim:(head + 1) * head_dim]
                if kind < 2:
                    one = one * cos_b + pltpu.roll(one, head_dim // 2, 1) * sin_b
                (dq, ktok_ref, vtok_ref)[kind][head] = one.astype(jnp.bfloat16).astype(jnp.bfloat16 if kind == 0 else jnp.float32)

    row_id = lax.broadcasted_iota(jnp.int32, (d_rows, 1), 0)

    def over_rows(src, body):
        def step(b, carry):
            slot = lax.rem(b, 2)
            c_copy(src, b, slot).wait()

            @pl.when(b + 1 < d_rows)
            def _():
                c_copy(src, b + 1, 1 - slot).start()

            body(b, slot)
            return carry

        lax.fori_loop(0, d_rows, step, 0)

    def decode_scores():
        def body(b, slot):
            for head in range(d_heads):
                sc = lax.dot_general(dq[head], cbuf[slot, head], nt, preferred_element_type=jnp.float32)
                dscr[head] = jnp.where(row_id == b, sc, dscr[head])

        over_rows(kc_hbm, body)
        c_copy(vc_hbm, 0, 0).start()
        scale = head_dim ** -0.5
        pos = lax.broadcasted_iota(jnp.int32, (d_rows, cache_len), 1)
        seen = pos < len_ref[...]
        for head in range(d_heads):
            sc = jnp.where(seen, dscr[head] * scale, MASKED)
            own_sc = jnp.sum(dq[head].astype(jnp.float32) * ktok_ref[head].astype(jnp.float32), axis=-1, keepdims=True) * scale
            top = jnp.maximum(jnp.max(sc, axis=-1, keepdims=True), own_sc)
            ex = jnp.exp(sc - top)
            own_ex = jnp.exp(own_sc - top)
            den = jnp.sum(ex, axis=-1, keepdims=True) + own_ex
            dprob[head] = (ex / den).astype(jnp.bfloat16)
            own_p = (own_ex / den).astype(jnp.bfloat16).astype(jnp.float32)
            dctx[:, head * head_dim:(head + 1) * head_dim] = own_p * vtok_ref[head].astype(jnp.float32)

    def decode_context():
        def body(b, slot):
            for head in range(d_heads):
                got = jnp.dot(dprob[head], cbuf[slot, head], preferred_element_type=jnp.float32)
                hc = slice(head * head_dim, (head + 1) * head_dim)
                dctx[:, hc] += jnp.where(row_id == b, got, 0.0)

        over_rows(vc_hbm, body)
        wo_lo.wait()
        wo_hi.wait()
        ctx_b = dctx[...].astype(jnp.bfloat16)
        val = jnp.dot(ctx_b[:, :lo_rows], gu_v[0, k_half:k_half + lo_rows, :], preferred_element_type=jnp.float32)
        dpart[0] = val + jnp.dot(ctx_b[:, lo_rows:], gu_v[1, k_half:k_half + shard - lo_rows, :], preferred_element_type=jnp.float32)
        for p in range(len(pieces)):
            gud_copy(p, 0).start()
            gud_copy(p, 1).start()

    base_d = base + 24
    d_cols = lambda d: pl.ds(pl.multiple_of(tp_of(d) * shard, 128), shard)

    def d_scatter(n, d):
        return remote(base_d + 6 * n + d - 1, dpart.at[n, :, d_cols(d)], dland.at[n, d - 1], {'tp': tp_of(d)})

    def d_gather(n, d):
        return remote(base_d + 6 * n + 2 + d, dtok.at[n, :, d_cols(0)], dtok.at[n, :, d_cols(0)], {'tp': tp_of(d)})

    def d_gather_land(n, d):
        return remote(base_d + 6 * n + 2 + d, dtok.at[n, :, d_cols(-d)], dtok.at[n, :, d_cols(-d)], {'tp': tp_of(d)})

    def decode_scatter(n):
        for d in range(1, tp_size):
            start(d_scatter(n, d))

    def decode_sum(n, before):
        for d in range(1, tp_size):
            d_scatter(n, d).wait_recv()
        total = dpart[n, :, d_cols(0)]
        for d in range(1, tp_size):
            total = total + dland[n, d - 1]
        dtok[n, :, d_cols(0)] = add_residual(before[:, d_cols(0)], total.astype(jnp.bfloat16))
        for d in range(1, tp_size):
            start(d_gather(n, d))

    def decode_gathered(n):
        for d in range(1, tp_size):
            d_gather_land(n, d).wait_recv()

    def decode_gate_up(lo, hi):
        normed = rms_norm(dtok[0], dg_ref[1:2, :])
        for p in range(lo, hi):
            f, size = pieces[p]
            gud_copy(p, 0).wait()
            gud_copy(p, 1).wait()
            gate = lax.dot_general(normed, gu_v[0, f:f + size, :], nt, preferred_element_type=jnp.float32)
            up = lax.dot_general(normed, gu_v[1, f:f + size, :], nt, preferred_element_type=jnp.float32)
            gate = gate.astype(jnp.bfloat16).astype(jnp.float32)
            up = up.astype(jnp.bfloat16).astype(jnp.float32)
            dact[:, f:f + size] = (gate * jax.nn.sigmoid(gate) * up).astype(jnp.bfloat16)

    def decode_down():
        wdd_copy.wait()
        dpart[1] = jnp.dot(dact[...], wd_v[...], preferred_element_type=jnp.float32)

    event(0, 0)
    decode_qkv()
    event(0, 1)
    decode_scores()
    event(1, 0)
    for n in range(2):
        far_send(n).wait_recv()
        start(far_relay(n))
    decode_context()
    decode_scatter(0)
    event(1, 1)

    base_ag = base + 12
    h_copy.wait()

    def ag(way, q, dev_i):
        idx = base_ag + 4 * way + 2 * q + dev_i
        return remote(idx, hb.at[:, cols(way, q)], out_hbm.at[rows_of(0), cols(way, q)], devs[dev_i])

    def ag_land(way, q, dev_i):
        idx = base_ag + 4 * way + 2 * q + dev_i
        return remote(idx, hb.at[:, cols(way, q)], out_hbm.at[rows_of(-1 if dev_i == 0 else 1), cols(way, q)], devs[dev_i])

    def fwd(way, q):
        ref = out_hbm.at[rows_of(-1 if way == 0 else 1), cols(way, q)]
        return remote(base_ag + 8 + 2 * way + q, ref, ref, devs[way])

    def fwd_land(way, q):
        ref = out_hbm.at[rows_of(2), cols(way, q)]
        return remote(base_ag + 8 + 2 * way + q, ref, ref, devs[way])

    for q in range(2):
        for way in range(2):
            rs(2, way, q).wait_recv()

            def end_step(i, carry, way=way, q=q):
                r = pl.ds(pl.multiple_of(i * nb, nb), nb)
                pr = pl.ds(pl.multiple_of(3 * chunk + i * nb, nb), nb)
                total = land[2, r, cols(way, q)] + part[pr, cols(way, q)]
                hb[r, cols(way, q)] = add_residual(hres[r, cols(way, q)], total.astype(jnp.bfloat16))
                return carry

            lax.fori_loop(0, chunk // nb, end_step, 0)
            start(ag(way, q, way))
            start(ag(way, q, 1 - way))
        if q == 0:
            decode_sum(0, tok_ref)
    own = pltpu.make_async_copy(hb, out_hbm.at[rows_of(0), :], osem.at[0])
    own.start()
    decode_gathered(0)
    mid = len(pieces) // 2
    for q in range(2):
        for way in range(2):
            ag_land(way, q, way).wait_recv()
            start(fwd(way, q))
        decode_gate_up(q * mid, mid if q == 0 else len(pieces))
    decode_down()
    decode_scatter(1)
    decode_sum(1, dtok.at[0])
    for q in range(2):
        for way in range(2):
            ag_land(way, q, 1 - way).wait_recv()
    for i in range(heads):
        if i != far:
            kv_land(i, k_hbm, kp_hbm, i).wait_recv()
            kv_land(i, v_hbm, vp_hbm, heads + i).wait_recv()
    for n in range(2):
        far_land(n).wait_recv()
    for q in range(2):
        for way in range(2):
            fwd_land(way, q).wait_recv()
    own.wait()
    decode_gathered(1)
    dec_ref[...] = dtok[1]
    for copy in sent:
        copy.wait_send()


def back_call(h, normed, w_gu, w_down, k, v, dec, tp_size, side_size):
    rows, depth = h.shape
    ff = w_down.shape[0]
    heads = k.shape[0]
    chunk = rows // tp_size
    fb = 256
    n_piece = -(-ff // fb)
    n_msg = 2 * heads + 12 + 12 + 12 + 2
    d_rows = dec[0].shape[0]
    head_dim = k.shape[2]
    cache_len = dec[9].shape[2]
    dma = pltpu.SemaphoreType.DMA
    bf16 = jnp.bfloat16
    kv = jax.ShapeDtypeStruct(k.shape, bf16)
    return pl.pallas_call(
        functools.partial(back_kernel, fb=fb, tp_size=tp_size, side_size=side_size),
        out_shape=(jax.ShapeDtypeStruct((rows, depth), bf16), kv, kv, jax.ShapeDtypeStruct((d_rows, depth), bf16)) + (jax.ShapeDtypeStruct((heads, d_rows, head_dim), jnp.float32),) * 2,
        in_specs=[ANY] * 6 + [VM] * 5 + [ANY] * 6,
        out_specs=(ANY,) * 3 + (VM,) * 3,
        scratch_shapes=[
            pltpu.VMEM((rows, depth), bf16),
            pltpu.VMEM((2 * chunk, ff), bf16),
            pltpu.VMEM((2, ff, depth), bf16),
            pltpu.VMEM((ff, depth), bf16),
            pltpu.VMEM((rows, depth), jnp.float32),
            pltpu.VMEM((3, chunk, depth), jnp.float32),
            pltpu.VMEM((chunk, depth), bf16),
            pltpu.VMEM((chunk, depth), bf16),
            pltpu.VMEM((2, rows, head_dim), bf16),
            pltpu.VMEM((2, heads, cache_len, head_dim), bf16),
            pltpu.VMEM((heads, d_rows, cache_len), jnp.float32),
            pltpu.VMEM((heads, d_rows, head_dim), bf16),
            pltpu.VMEM((heads, d_rows, cache_len), bf16),
            pltpu.VMEM((d_rows, heads * head_dim), jnp.float32),
            pltpu.VMEM((2, d_rows, depth), jnp.float32),
            pltpu.VMEM((2, tp_size - 1, d_rows, heads * head_dim), jnp.float32),
            pltpu.VMEM((2, d_rows, depth), bf16),
            pltpu.VMEM((d_rows, ff), bf16),
            dma((tp_size,)), dma((2 * n_piece,)), dma((4,)), dma((1,)), dma((1,)), dma((6 * heads,)), dma((2 * n_piece,)), dma((2,)), dma((n_msg,)), dma((n_msg,)),
        ],
        compiler_params=pltpu.CompilerParams(vmem_limit_bytes=67043328, collective_id=1, has_side_effects=True),
        cost_estimate=pl.CostEstimate(flops=6 * rows * ff * depth, bytes_accessed=6 * ff * depth + 8 * rows * depth, transcendentals=0),
        name="back",
    )(h, normed, w_gu, w_down, k, v, *dec)


def cache_kernel(len_ref, kt_ref, vt_ref, k_ref, v_ref, ko_ref, vo_ref):
    n_rows, heads, cache_len, head_dim = k_ref.shape
    first = pl.program_id(0) * n_rows
    tile = 16
    pos = lax.broadcasted_iota(jnp.int32, (tile, head_dim), 0)
    ko_ref[...] = k_ref[...]
    vo_ref[...] = v_ref[...]
    for j in range(n_rows):
        at = len_ref[first + j]
        base = pl.multiple_of(at // tile * tile, tile)
        here = pos == at - base
        for head in range(heads):
            for tok, src, dst in ((kt_ref, k_ref, ko_ref), (vt_ref, v_ref, vo_ref)):
                new = tok[head, pl.ds(first + j, 1), :]
                old = src[j, head, pl.ds(base, tile), :].astype(jnp.float32)
                dst[j, head, pl.ds(base, tile), :] = jnp.where(here, new, old).astype(dst.dtype)


def cache_call(c_len, k_tok, v_tok, k_cache, v_cache):
    d_rows, heads, cache_len, head_dim = k_cache.shape
    step = 2
    block = pl.BlockSpec((step, heads, cache_len, head_dim), lambda i: (i, 0, 0, 0))
    out = jax.ShapeDtypeStruct(k_cache.shape, k_cache.dtype)
    return pl.pallas_call(
        cache_kernel,
        grid=(d_rows // step,),
        out_shape=(out, out),
        in_specs=[SM, VM, VM, block, block],
        out_specs=(block, block),
        compiler_params=pltpu.CompilerParams(vmem_limit_bytes=67043328),
        cost_estimate=pl.CostEstimate(flops=k_cache.size, bytes_accessed=8 * k_cache.size, transcendentals=0),
        name="cache",
    )(c_len, k_tok, v_tok, k_cache, v_cache)


def run_layers(prompt, s_len, pre, tokens, k_cache, v_cache, c_len, dec, tp_size, side_size):
    w_qkv, w_out, w_gu, w_down, gains = pre
    dw_qkv, dw_out, dw_gu, dw_down, dgains = dec
    rows, width = prompt.shape
    layers, _, _, heads_loc, head_dim = w_qkv.shape
    shard = heads_loc * head_dim
    d_rows, cache_len = k_cache.shape[1:3]

    cos_tab, sin_tab = rope_tables(jnp.concatenate([jnp.arange(rows, dtype=jnp.int32), c_len]), head_dim)
    cos_full = jnp.concatenate([cos_tab, cos_tab], axis=-1)
    sin_full = jnp.concatenate([-sin_tab, sin_tab], axis=-1)
    hidden = prompt
    outs = []
    for layer in range(layers):
        w_t = w_qkv[layer].transpose(1, 2, 0, 3)
        hidden, normed, k, v = front_call(hidden, s_len, gains[layer], cos_full, sin_full, w_t, w_out[layer].reshape(shard, width), tp_size, side_size)
        by_head = lambda cache: cache[layer].reshape(d_rows, cache_len, heads_loc, head_dim).transpose(0, 2, 1, 3)
        dec_args = (tokens, c_len[:, None], cos_full, sin_full, dgains[layer], dw_qkv[layer].reshape(width, 3, heads_loc, head_dim).transpose(1, 2, 0, 3), dw_out[layer].reshape(shard, width), dw_gu[layer], dw_down[layer], by_head(k_cache), by_head(v_cache))
        hidden, k_inst, v_inst, tokens, k_tok, v_tok = back_call(hidden, normed, w_gu[layer], w_down[layer], k, v, dec_args, tp_size, side_size)
        k_new, v_new = cache_call(c_len, k_tok, v_tok, by_head(k_cache), by_head(v_cache))
        as_cache = lambda new: new.transpose(0, 2, 1, 3)[:, :, :, None, :]
        outs.append((k_inst.transpose(1, 0, 2)[:, :, None, :], v_inst.transpose(1, 0, 2)[:, :, None, :], as_cache(k_new), as_cache(v_new)))
    return (hidden, tokens) + tuple(jnp.stack(parts) for parts in zip(*outs))


def solution(mesh):
    tp_size = mesh.shape['tp']
    side_size = mesh.shape['side']
    inst_axes = ('pair', 'side')
    rows_spec = P(inst_axes, None)
    vec_spec = P(inst_axes)
    cache_spec = P(None, inst_axes, None, None, 'tp', None)
    prompt_spec = P(None, inst_axes, None, 'tp', None)
    in_specs = (rows_spec, vec_spec, P(None, None, None, 'tp', None), P(None, 'tp', None, None), P(None, None, 'tp', None), P(None, 'tp', None), P(None, None, None), rows_spec, cache_spec, cache_spec, vec_spec, P(None, None, None, None, 'tp', None), P(None, None, 'tp', None, None), P(None, None, 'tp', None), P(None, 'tp', None), P(None, None, None))
    out_specs = (rows_spec, rows_spec, prompt_spec, prompt_spec, cache_spec, cache_spec)

    def device_fn(prompt_x, s_len, w_qkv_pre, w_out_pre, w_gu_pre, w_down_pre, gain_pre, dec_tokens, k_cache, v_cache, c_len, w_qkv_dec, w_out_dec, w_gu_dec, w_down_dec, gain_dec):
        pre = (w_qkv_pre, w_out_pre, w_gu_pre, w_down_pre, gain_pre)
        dec = (w_qkv_dec, w_out_dec, w_gu_dec, w_down_dec, gain_dec)
        return run_layers(prompt_x, s_len, pre, dec_tokens, k_cache, v_cache, c_len, dec, tp_size, side_size)

    return jax.shard_map(device_fn, mesh=mesh, in_specs=in_specs, out_specs=out_specs, check_vma=False)
```
